256 devices in a mesh: ens: 8 (over y_hi, x), lon: 32 (over z, y_lo, core).
Axes of the slice: x: 4, y: 4 (y_hi: 2, y_lo: 2; y = y_hi * 2 + y_lo), z: 8, core: 2. Of those that a mesh axis runs over, the one named last changes fastest.
Arguments:
- control: float32 [16, 1024, 2048], P('ens', None, 'lon'), may hold values from -6 to 6
- residual: float32 [16, 1024, 2048], P('ens', None, 'lon'), may hold values from -6 to 6
- direction: float32 [16, 1024, 2048], P('ens', None, 'lon'), may hold values from -6 to 6
- ens_perturb: bfloat16 [16, 3, 1024, 2048], P('ens', None, None, 'lon'), may hold values from -1.5 to 1.5
- localize: float32 [1024, 1024], replicated, may hold values from -0.5 to 1.5
- obs_cell: int32 [131072], P('lon'), may hold values from 0 to 65535
- obs_slot: int32 [131072], P('lon'), may hold values from 0 to 3
- obs_weight: float32 [131072], P('lon'), may hold values from 0.5 to 4
Outputs:
- control_new: float32 [16, 1024, 2048], P('ens', None, 'lon')
- residual_new: float32 [16, 1024, 2048], P('ens', None, 'lon')
- direction_new: float32 [16, 1024, 2048], P('ens', None, 'lon')
The draws below stay inside these ranges and needn't reach their ends.
Inputs may be any that keep to these rules, and one draw needn't show every extreme that they name: `obs_cell`: row-major cell within the entry's own longitude tile: row times 64 plus column. `obs_slot`: slot n < 3 observes the height after model step n + 1; slot 3 marks a padding entry that observes nothing.
All inputs are finite; a program needn't handle non-finite values.
Results may differ from the reference program's by a relative error of at most 0.0003.
Values sent between devices are 32-bit elements; how exact they have to be, the bound alone decides.
No kernel may reach another device: no remote copies, remote signals or barrier semaphores. Data moves between devices by JAX's collectives and lax.ppermute only.
A program may use at most 64 MiB of HBM per device.

```python
import math
import jax
import jax.numpy as jnp
from jax import lax

LAT = 1024
CLON = 64
STEPS = 3
NOBS_DEV = 4096
MEMBERS = 16
LON = 2048
NOBS = 131072


def draw_localize(key, part):
    row_ids = jnp.arange(LAT).astype(jnp.float32)
    distance = jnp.abs(row_ids[:, None] - row_ids[None, :])
    envelope = jnp.exp(-distance * 8.0 / LAT)
    jitter = 0.15 * jax.random.normal(key, (LAT, LAT), jnp.float32)
    jitter = jnp.clip(jitter, -0.5, 0.5)
    return jnp.eye(LAT, dtype=jnp.float32) + envelope * jitter


def place_ends(result, key, least, top_value):
    spot = [jax.random.randint(jax.random.fold_in(key, axis), (), 0, length) for axis, length in enumerate(result.shape)]
    main_axis = result.shape.index(max(result.shape))
    neighbour = spot[:main_axis] + [(spot[main_axis] + 1) % result.shape[main_axis]] + spot[main_axis + 1:]
    return result.at[tuple(spot)].set(least).at[tuple(neighbour)].set(top_value)


def levels(own_key, shape, split, least, largest):
    gain, own = 1.0, jax.random.fold_in(own_key, 6)
    for axis_at, blocks in split:
        draws = jnp.exp(jax.random.uniform(jax.random.fold_in(own, axis_at), (blocks,), jnp.float32, least / len(split), largest / len(split)))
        gain = gain * jnp.repeat(draws, shape[axis_at] // blocks).reshape([-1 if axis == axis_at else 1 for axis in range(len(shape))])
    return gain


def normal_values(own_key, dims, deviation, bound, split=(), held_as=jnp.bfloat16):
    gain = levels(own_key, dims, split, -0.22, 0.18) if split else 1.0
    result = jax.random.normal(own_key, dims, jnp.float32) * deviation * gain
    return jnp.minimum(jnp.maximum(result, -bound), bound).astype(held_as)


def setup_inputs(seed: int = 0) -> dict:
    keys = jax.random.split(jax.random.key(seed), 9)
    control = normal_values(keys[0], (MEMBERS, LAT, LON), 1.0, 6.0, ((0, 8), (2, 32)), jnp.float32)
    residual = normal_values(keys[1], (MEMBERS, LAT, LON), 1.0, 6.0, ((0, 8), (2, 32)), jnp.float32)
    direction = normal_values(keys[2], (MEMBERS, LAT, LON), 1.0, 6.0, ((0, 8), (2, 32)), jnp.float32)
    ens_perturb = normal_values(keys[3], (MEMBERS, 3, LAT, LON), 0.25, 1.5, ((0, 8), (3, 32)))
    localize = draw_localize(jax.random.fold_in(keys[8], 71), 0)
    obs_cell = place_ends(jax.random.randint(keys[5], (NOBS,), 0, LAT * CLON), jax.random.fold_in(keys[5], 1), 0, (LAT * CLON) - 1).astype(jnp.int32)
    obs_slot = place_ends(jax.random.randint(keys[6], (NOBS,), 0, STEPS + 1), jax.random.fold_in(keys[6], 1), 0, STEPS).astype(jnp.int32)
    obs_weight = jnp.clip(jnp.exp(math.log(4.0) - 2.0794415 * jax.random.uniform(keys[7], (NOBS,), jnp.float32) ** levels(keys[7], (NOBS,), ((0, 32),), -0.2, 0.2)), 0.5, 4.0)
    return {"control": control, "residual": residual, "direction": direction, "ens_perturb": ens_perturb, "localize": localize, "obs_cell": obs_cell, "obs_slot": obs_slot, "obs_weight": obs_weight}


wave_speed = 0.35
rotation = 0.2

def grid_factors(row_ids, lat_total):
    latitude = (-1.0 / 3.0 + 2.0 / 3.0 * (row_ids + 0.5) / lat_total) * jnp.pi
    return (1.0 / jnp.cos(latitude), jnp.sin(latitude))

def linear_step(fields, orient, metric, coriolis):
    height, zonal, meridional = (fields[0], fields[1], fields[2])

    def lon_diff(values):
        return 0.5 * metric[:, None] * (jnp.roll(values, -1, axis=1) - jnp.roll(values, 1, axis=1))

    def lat_diff(values):
        widened = jnp.pad(values, ((1, 1), (0, 0)))
        return 0.5 * (widened[2:] - widened[:-2])
    speed = orient * wave_speed
    turning = orient * rotation * coriolis[:, None]
    return jnp.stack([height - speed * (lon_diff(zonal) + lat_diff(meridional)), zonal - speed * lon_diff(height) + turning * meridional, meridional - speed * lat_diff(height) - turning * zonal])

def reference(control, residual, direction, ens_perturb, localize, obs_cell, obs_slot, obs_weight):
    hi = lax.Precision.HIGHEST
    row_ids = jnp.arange(LAT).astype(jnp.float32)
    metric, coriolis = grid_factors(row_ids, LAT)
    tile_index = (jnp.arange(obs_cell.shape[0]) // NOBS_DEV).astype(jnp.int32)
    cell_index = (obs_cell // CLON * LON + tile_index * CLON + obs_cell % CLON).astype(jnp.int32)

    def member_inc(accum, member_pair):
        member_pert, member_vec = member_pair
        localized = jnp.dot(localize, member_vec, precision=hi)
        return (accum + member_pert.astype(jnp.float32) * localized[None], None)
    increment, _ = lax.scan(member_inc, jnp.zeros((3, LAT, LON), jnp.float32), (ens_perturb, direction))
    tl_state = increment
    observed = jnp.zeros(obs_cell.shape, jnp.float32)
    for moment in range(STEPS):
        tl_state = linear_step(tl_state, 1.0, metric, coriolis)
        sampled = tl_state[0].reshape(-1)[cell_index]
        observed = jnp.where(obs_slot == moment, sampled, observed)
    weighted = obs_weight * observed
    adjoint = jnp.zeros((3, LAT, LON), jnp.float32)
    for moment in reversed(range(STEPS)):
        forcing = jnp.zeros((LAT * LON,), jnp.float32).at[cell_index].add(jnp.where(obs_slot == moment, weighted, 0.0))
        adjoint = adjoint.at[0].add(forcing.reshape(LAT, LON))
        adjoint = linear_step(adjoint, -1.0, metric, coriolis)

    def member_grad(carried, member_pert):
        projected = lax.optimization_barrier(jnp.sum(member_pert.astype(jnp.float32) * adjoint, axis=0))
        return (carried, jnp.dot(localize.T, projected, precision=hi))
    _, pulled_back = lax.scan(member_grad, jnp.float32(0.0), ens_perturb)
    image_vec = direction + pulled_back
    norm_old = jnp.sum(residual * residual)
    step_size = norm_old / jnp.sum(direction * image_vec)
    control_new = control + step_size * direction
    residual_new = residual - step_size * image_vec
    norm_new = jnp.sum(residual_new * residual_new)
    direction_new = residual_new + norm_new / norm_old * direction
    return (control_new, residual_new, direction_new)
```

```python
import functools

import jax
import jax.numpy as jnp
import numpy as np
from jax import lax
from jax.experimental import pallas as pl
from jax.experimental.pallas import tpu as pltpu
from jax.sharding import Mesh
from jax.sharding import PartitionSpec as P

STEPS = 3
HALO = 3
PAD = 8
LON = ("lon_0", "lon_1", "lon_2")
ENS = ("ens_0", "ens_1")
ENS_LON = ("ens_0", "ens_1", "lon_0", "lon_1", "lon_2")

wave_speed = 0.35
rotation = 0.2

F32 = jnp.float32
BF16 = jnp.bfloat16
NT = (((1,), (1,)), ((), ()))
NN = (((1,), (0,)), ((), ()))


def split_two(x):
    high = x.astype(BF16)
    low = (x - high.astype(F32)).astype(BF16)
    return high, low


def dot(a, b, dims):
    return lax.dot_general(a, b, dims, preferred_element_type=F32)


def grid_factors(lat_total):
    row_ids = np.arange(lat_total).astype(np.float32)
    latitude = (-1.0 / 3.0 + 2.0 / 3.0 * (row_ids + 0.5) / lat_total) * np.pi
    return np.stack([1.0 / np.cos(latitude), np.sin(latitude)]).astype(np.float32)


def model_step(h, u, v, orient, metric, coriolis):
    wide, rows = h.shape
    lane = lax.broadcasted_iota(jnp.int32, (1, rows), 1)
    lon_scale = (orient * wave_speed * 0.5) * metric
    lat_scale = orient * wave_speed * 0.5
    turn = (orient * rotation) * coriolis
    keep_next = jnp.where(lane == rows - 1, 0.0, lat_scale)
    keep_last = jnp.where(lane == 0, 0.0, lat_scale)

    def lon_diff(x):
        return lon_scale * (pltpu.roll(x, wide - 1, 0) - pltpu.roll(x, 1, 0))

    def lat_diff(x):
        return keep_next * pltpu.roll(x, rows - 1, 1) - keep_last * pltpu.roll(x, 1, 1)

    return (
        h - (lon_diff(u) + lat_diff(v)),
        u - lon_diff(h) + turn * v,
        v - lat_diff(h) - turn * u,
    )


def increment_kernel(loc_ref, dir_ref, pert_ref, inc_ref, left_ref, right_ref, parts_ref):
    members, cols, rows = dir_ref.shape
    lines = members * cols

    @pl.when(pl.program_id(0) == 0)
    def _():
        high, low = split_two(dir_ref[...].reshape(lines, rows))
        parts_ref[0:lines] = high
        parts_ref[lines : 2 * lines] = low

    loc_high, loc_low = split_two(loc_ref[...])
    both = dot(parts_ref[...], loc_high, NT)
    rest = dot(parts_ref[0:lines], loc_low, NT)
    localized = both[0:lines] + both[lines : 2 * lines] + rest
    for field in range(3):
        total = None
        for m in range(members):
            term = pert_ref[m, field].astype(F32) * localized[m * cols : (m + 1) * cols]
            total = term if total is None else total + term
        inc_ref[field] = total
        left_ref[HALO * field : HALO * (field + 1)] = total[0:HALO]
        right_ref[HALO * field : HALO * (field + 1)] = total[cols - HALO : cols]


def partial_increment(localize, direction, pert):
    members, cols, rows = direction.shape
    block = 256
    edge = jax.ShapeDtypeStruct((3 * HALO, rows), F32)
    edge_spec = pl.BlockSpec((3 * HALO, block), lambda i: (0, i))
    return pl.pallas_call(
        increment_kernel,
        grid=(rows // block,),
        in_specs=[
            pl.BlockSpec((block, rows), lambda i: (i, 0)),
            pl.BlockSpec((members, cols, rows), lambda i: (0, 0, 0)),
            pl.BlockSpec((members, 3, cols, block), lambda i: (0, 0, 0, i)),
        ],
        out_specs=[pl.BlockSpec((3, cols, block), lambda i: (0, 0, i)), edge_spec, edge_spec],
        out_shape=[jax.ShapeDtypeStruct((3, cols, rows), F32), edge, edge],
        scratch_shapes=[pltpu.VMEM((2 * members * cols, rows), BF16)],
        name="increment",
    )(localize, direction, pert)


def forward_kernel(
    inc_ref, west_ref, east_ref, factor_ref, row_ref, spot_ref, out_ref, state_ref, parts_ref
):
    _, cols, rows = inc_ref.shape
    nobs = row_ref.shape[1]
    wide = cols + 2 * PAD
    state_ref[...] = jnp.zeros(state_ref.shape, F32)
    for field in range(3):
        lines = slice(HALO * field, HALO * (field + 1))
        state_ref[field, PAD : PAD + cols] = inc_ref[field]
        state_ref[field, PAD - HALO : PAD] = west_ref[lines]
        state_ref[field, PAD + cols : PAD + cols + HALO] = east_ref[lines]
    metric = factor_ref[0:1]
    coriolis = factor_ref[1:2]
    spots = STEPS * cols
    for moment in range(STEPS):
        h, u, v = model_step(state_ref[0], state_ref[1], state_ref[2], 1.0, metric, coriolis)
        state_ref[0] = h
        state_ref[1] = u
        state_ref[2] = v
        high, low = split_two(h[PAD : PAD + cols])
        parts_ref[moment * cols : (moment + 1) * cols] = high
        parts_ref[spots + moment * cols : spots + (moment + 1) * cols] = low
    chunk = 512
    for start in range(0, nobs, chunk):
        here = slice(start, start + chunk)
        row_hot = lax.broadcasted_iota(jnp.int32, (rows, chunk), 0) == row_ref[:, here]
        picked = dot(parts_ref[...], row_hot.astype(F32).astype(BF16), NN)
        picked = picked[0:spots] + picked[spots : 2 * spots]
        spot_hot = lax.broadcasted_iota(jnp.int32, (spots, chunk), 0) == spot_ref[:, here]
        value = jnp.sum(jnp.where(spot_hot, picked, 0.0), axis=0, keepdims=True)
        out_ref[:, here] = jnp.broadcast_to(value, (out_ref.shape[0], chunk))


def observed_parts(inc, west, east, factors, obs_row, obs_spot, copies):
    _, cols, rows = inc.shape
    nobs = obs_row.shape[1]
    return pl.pallas_call(
        forward_kernel,
        out_shape=jax.ShapeDtypeStruct((copies, nobs), F32),
        scratch_shapes=[
            pltpu.VMEM((3, cols + 2 * PAD, rows), F32),
            pltpu.VMEM((2 * STEPS * cols, rows), BF16),
        ],
        name="forward",
    )(inc, west, east, factors, obs_row, obs_spot)


def adjoint_kernel(
    seen_ref, weight_ref, row_ref, spot_ref, factor_ref, adj_ref, left_ref, right_ref,
    state_ref, force_ref,
):
    _, cols, rows = adj_ref.shape
    nobs = row_ref.shape[1]
    spots = STEPS * cols
    chunk = 512
    for start in range(0, nobs, chunk):
        here = slice(start, start + chunk)
        weighted = weight_ref[:, here] * jnp.sum(seen_ref[:, here], axis=0, keepdims=True)
        spot_hot = lax.broadcasted_iota(jnp.int32, (spots, chunk), 0) == spot_ref[:, here]
        high, low = split_two(jnp.where(spot_hot, weighted, 0.0))
        row_hot = lax.broadcasted_iota(jnp.int32, (rows, chunk), 0) == row_ref[:, here]
        part = dot(
            jnp.concatenate([high, low], axis=0), row_hot.astype(F32).astype(BF16), NT
        )
        part = part[0:spots] + part[spots : 2 * spots]
        if start == 0:
            force_ref[...] = part
        else:
            force_ref[...] += part
    metric = factor_ref[0:1]
    coriolis = factor_ref[1:2]
    state_ref[...] = jnp.zeros(state_ref.shape, F32)
    for moment in reversed(range(STEPS)):
        state_ref[0, PAD : PAD + cols] += force_ref[moment * cols : (moment + 1) * cols]
        h, u, v = model_step(state_ref[0], state_ref[1], state_ref[2], -1.0, metric, coriolis)
        state_ref[0] = h
        state_ref[1] = u
        state_ref[2] = v
    for field in range(3):
        lines = slice(HALO * field, HALO * (field + 1))
        adj_ref[field] = state_ref[field, PAD : PAD + cols]
        left_ref[lines] = state_ref[field, PAD - HALO : PAD]
        right_ref[lines] = state_ref[field, PAD + cols : PAD + cols + HALO]


def tile_adjoint(seen, weight, obs_row, obs_spot, factors, cols):
    rows = factors.shape[1]
    edge = jax.ShapeDtypeStruct((3 * HALO, rows), F32)
    return pl.pallas_call(
        adjoint_kernel,
        out_shape=[jax.ShapeDtypeStruct((3, cols, rows), F32), edge, edge],
        scratch_shapes=[
            pltpu.VMEM((3, cols + 2 * PAD, rows), F32),
            pltpu.VMEM((STEPS * cols, rows), F32),
        ],
        name="adjoint",
    )(seen, weight, obs_row, obs_spot, factors)


def image_kernel(
    loc_ref, adj_ref, west_ref, east_ref, pert_ref, dir_ref, res_ref, img_ref, sums_ref,
    parts_ref, total_ref,
):
    members, cols, rows = pert_ref.shape[0], pert_ref.shape[2], pert_ref.shape[3]
    block = loc_ref.shape[1]
    lines = members * cols
    step = pl.program_id(0)

    @pl.when(step == 0)
    def _():
        total_ref[...] = jnp.zeros(total_ref.shape, F32)
        adj = []
        for field in range(3):
            edges = slice(HALO * field, HALO * (field + 1))
            middle = jnp.zeros((cols - 2 * HALO, rows), F32)
            extra = jnp.concatenate([west_ref[edges], middle, east_ref[edges]], axis=0)
            adj.append(adj_ref[field] + extra)
        for m in range(members):
            projected = pert_ref[m, 0].astype(F32) * adj[0]
            projected += pert_ref[m, 1].astype(F32) * adj[1]
            projected += pert_ref[m, 2].astype(F32) * adj[2]
            high, low = split_two(projected)
            parts_ref[m * cols : (m + 1) * cols] = high
            parts_ref[lines + m * cols : lines + (m + 1) * cols] = low

    loc_high, loc_low = split_two(loc_ref[...])
    both = dot(parts_ref[...], loc_high, NN)
    rest = dot(parts_ref[0:lines], loc_low, NN)
    pulled = both[0:lines] + both[lines : 2 * lines] + rest
    way = dir_ref[...].reshape(lines, block)
    left = res_ref[...].reshape(lines, block)
    image = way + pulled
    img_ref[...] = image.reshape(members, cols, block)

    def fold(x):
        x = jnp.sum(x.reshape(lines // 8, 8, block), axis=0)
        return sum(x[:, i : i + 128] for i in range(0, block, 128))

    total_ref[0] += fold(left * left)
    total_ref[1] += fold(way * image)
    total_ref[2] += fold(left * image)
    total_ref[3] += fold(image * image)

    @pl.when(step == pl.num_programs(0) - 1)
    def _():
        lane = lax.broadcasted_iota(jnp.int32, (1, 128), 1)
        packed = jnp.zeros((1, 128), F32)
        for i in range(4):
            packed = jnp.where(lane == i, jnp.sum(total_ref[i]), packed)
        sums_ref[...] = jnp.broadcast_to(packed, sums_ref.shape)


def image_and_sums(localize, adj, west, east, pert, direction, residual, copies):
    members, _, cols, rows = pert.shape
    block = 256
    whole = lambda *dims: pl.BlockSpec(dims, lambda i: (0,) * len(dims))
    part = pl.BlockSpec((members, cols, block), lambda i: (0, 0, i))
    return pl.pallas_call(
        image_kernel,
        grid=(rows // block,),
        in_specs=[
            pl.BlockSpec((rows, block), lambda i: (0, i)),
            whole(3, cols, rows),
            whole(3 * HALO, rows),
            whole(3 * HALO, rows),
            whole(members, 3, cols, rows),
            part,
            part,
        ],
        out_specs=[part, whole(copies, 128)],
        out_shape=[
            jax.ShapeDtypeStruct((members, cols, rows), F32),
            jax.ShapeDtypeStruct((copies, 128), F32),
        ],
        scratch_shapes=[
            pltpu.VMEM((2 * members * cols, rows), BF16),
            pltpu.VMEM((4, 8, 128), F32),
        ],
        name="image",
    )(localize, adj, west, east, pert, direction, residual)


def neighbours(to_west, to_east):
    count = lax.axis_size(LON)
    east = [(i, (i + 1) % count) for i in range(count)]
    west = [(target, source) for source, target in east]
    from_west = lax.ppermute(to_east, LON, east)
    from_east = lax.ppermute(to_west, LON, west)
    return from_west, from_east


def body(control, residual, direction, ens_perturb, localize, obs_cell, obs_slot, obs_weight):
    lat_total = localize.shape[0]
    cols = control.shape[2]
    factors = jnp.asarray(grid_factors(lat_total))
    turned = lambda x: jnp.swapaxes(x, 1, 2)
    control_t, residual_t, direction_t = turned(control), turned(residual), turned(direction)
    pert = jnp.swapaxes(ens_perturb, 2, 3)
    obs_row = (obs_cell // cols)[None]
    obs_spot = (obs_slot * cols + obs_cell % cols)[None]
    inc, left, right = partial_increment(localize, direction_t, pert)
    west, east = neighbours(left, right)
    copies = lax.axis_size(ENS)
    seen = observed_parts(inc, west, east, factors, obs_row, obs_spot, copies)
    seen = lax.all_to_all(seen, ENS, 0, 0, tiled=True)
    adj, left, right = tile_adjoint(seen, obs_weight[None], obs_row, obs_spot, factors, cols)
    west, east = neighbours(left, right)
    image, sums = image_and_sums(
        localize, adj, west, east, pert, direction_t, residual_t, lax.axis_size(ENS_LON)
    )
    sums = jnp.sum(lax.all_to_all(sums, ENS_LON, 0, 0, tiled=True), axis=0)
    norm_old, curvature, cross_term, square = sums[0], sums[1], sums[2], sums[3]
    step_size = norm_old / curvature
    norm_new = norm_old - 2.0 * step_size * cross_term + step_size * step_size * square
    control_new = control_t + step_size * direction_t
    residual_new = residual_t - step_size * image
    direction_new = residual_new + norm_new / norm_old * direction_t
    return (turned(control_new), turned(residual_new), turned(direction_new))


def solution(mesh):
    split = Mesh(mesh.devices.reshape(2, 4, 8, 2, 2), ("ens_0", "ens_1", "lon_0", "lon_1", "lon_2"))
    placed = (
        P(ENS, None, LON),
        P(ENS, None, LON),
        P(ENS, None, LON),
        P(ENS, None, None, LON),
        P(),
        P(LON),
        P(LON),
        P(LON),
    )
    return jax.shard_map(
        body,
        mesh=split,
        in_specs=placed,
        out_specs=(P(ENS, None, LON), P(ENS, None, LON), P(ENS, None, LON)),
        check_vma=False,
    )
```

```python
import functools

import jax
import jax.numpy as jnp
import numpy as np
from jax import lax
from jax.experimental import pallas as pl
from jax.experimental.pallas import tpu as pltpu
from jax.sharding import Mesh
from jax.sharding import PartitionSpec as P

STEPS = 3
HALO = 3
PAD = 8
LON = ("lon_0", "lon_1", "lon_2")
ENS = ("ens_0", "ens_1")
ENS_LON = ("ens_0", "ens_1", "lon_0", "lon_1", "lon_2")

wave_speed = 0.35
rotation = 0.2

F32 = jnp.float32
BF16 = jnp.bfloat16
NT = (((1,), (1,)), ((), ()))
NN = (((1,), (0,)), ((), ()))
HBM = pl.BlockSpec(memory_space=pltpu.HBM)


def split_two(x):
    high = x.astype(BF16)
    low = (x - high.astype(F32)).astype(BF16)
    return high, low


def dot(a, b, dims):
    return lax.dot_general(a, b, dims, preferred_element_type=F32)


def grid_factors(lat_total):
    row_ids = np.arange(lat_total).astype(np.float32)
    latitude = (-1.0 / 3.0 + 2.0 / 3.0 * (row_ids + 0.5) / lat_total) * np.pi
    return np.stack([1.0 / np.cos(latitude), np.sin(latitude)]).astype(np.float32)


def model_step(h, u, v, orient, metric, coriolis):
    wide, rows = h.shape
    lane = lax.broadcasted_iota(jnp.int32, (1, rows), 1)
    lon_scale = (orient * wave_speed * 0.5) * metric
    lat_scale = orient * wave_speed * 0.5
    turn = (orient * rotation) * coriolis
    keep_next = jnp.where(lane == rows - 1, 0.0, lat_scale)
    keep_last = jnp.where(lane == 0, 0.0, lat_scale)

    def lon_diff(x):
        return lon_scale * (pltpu.roll(x, wide - 1, 0) - pltpu.roll(x, 1, 0))

    def lat_diff(x):
        return keep_next * pltpu.roll(x, rows - 1, 1) - keep_last * pltpu.roll(x, 1, 1)

    return (
        h - (lon_diff(u) + lat_diff(v)),
        u - lon_diff(h) + turn * v,
        v - lat_diff(h) - turn * u,
    )


def call(kernel, name, out_shape, scratch, flops, limit_mib=24, **options):
    return pl.pallas_call(
        kernel,
        name=name,
        out_shape=out_shape,
        scratch_shapes=scratch,
        compiler_params=pltpu.CompilerParams(vmem_limit_bytes=limit_mib << 20),
        cost_estimate=pl.CostEstimate(flops=flops, bytes_accessed=1 << 20, transcendentals=0),
        **options,
    )


def floats(*dims):
    return jax.ShapeDtypeStruct(dims, F32)


def rows_and_spots(cell, slot, cols):
    bits = cols.bit_length() - 1
    assert cols == 1 << bits
    return lax.shift_right_logical(cell, bits), slot, cell & (cols - 1)


def one_hot_rows(row, rows):
    ids = lax.broadcasted_iota(jnp.int32, (rows, row.shape[1]), 0)
    return (ids == row).astype(F32).astype(BF16)


def edges_of(field):
    return slice(HALO * field, HALO * (field + 1))


def increment_kernel(
    loc_hbm, dir_hbm, pert_hbm, inc_ref, left_ref, right_ref, high_ref, low_ref,
    loc_ref, dir_ref, pert_ref, parts_ref, sems,
):
    members, cols, rows = dir_ref.shape
    lines = members * cols
    block = 256
    blocks = rows // block
    first = pltpu.make_async_copy(dir_hbm, dir_ref, sems.at[0])
    first.start()
    copies = []
    for i in range(blocks):
        here = slice(i * block, (i + 1) * block)
        copies.append(
            pltpu.make_async_copy(loc_hbm.at[here], loc_ref.at[here], sems.at[2 + i])
        )
    copies[0].start()
    second = pltpu.make_async_copy(pert_hbm, pert_ref, sems.at[1])
    second.start()
    for copy in copies[1:]:
        copy.start()
    first.wait()
    high, low = split_two(dir_ref[...].reshape(lines, rows))
    parts_ref[0:lines] = high
    parts_ref[lines : 2 * lines] = low
    for i in range(blocks):
        here = slice(i * block, (i + 1) * block)
        copies[i].wait()
        loc_high, loc_low = split_two(loc_ref[here])
        high_ref[here] = loc_high
        low_ref[here] = loc_low
        both = dot(parts_ref[...], loc_high, NT)
        rest = dot(parts_ref[0:lines], loc_low, NT)
        localized = both[0:lines] + both[lines : 2 * lines] + rest
        if i == 0:
            second.wait()
        for field in range(3):
            total = None
            for m in range(members):
                term = pert_ref[m, field, :, here].astype(F32) * localized[m * cols : (m + 1) * cols]
                total = term if total is None else total + term
            inc_ref[field, :, here] = total
            left_ref[edges_of(field), here] = total[0:HALO]
            right_ref[edges_of(field), here] = total[cols - HALO : cols]


def partial_increment(localize, direction, pert):
    members, cols, rows = direction.shape
    half = jax.ShapeDtypeStruct((rows, rows), BF16)
    return call(
        increment_kernel,
        "increment",
        [floats(3, cols, rows), floats(3 * HALO, rows), floats(3 * HALO, rows), half, half],
        [
            pltpu.VMEM((rows, rows), F32),
            pltpu.VMEM(direction.shape, F32),
            pltpu.VMEM(pert.shape, BF16),
            pltpu.VMEM((2 * members * cols, rows), BF16),
            pltpu.SemaphoreType.DMA((2 + rows // 256,)),
        ],
        10**9,
        in_specs=[HBM, HBM, HBM],
    )(*(pltpu.with_memory_space_constraint(x, pltpu.HBM) for x in (localize, direction, pert)))


def forward_kernel(inc_ref, factor_ref, cell_ref, slot_ref, out_ref, state_ref, parts_ref):
    _, cols, rows = inc_ref.shape
    nobs = cell_ref.shape[1]
    state_ref[...] = jnp.zeros(state_ref.shape, F32)
    for field in range(3):
        state_ref[field, PAD : PAD + cols] = inc_ref[field]
    metric = factor_ref[0:1]
    coriolis = factor_ref[1:2]
    spots = STEPS * cols
    for moment in range(STEPS):
        h, u, v = model_step(state_ref[0], state_ref[1], state_ref[2], 1.0, metric, coriolis)
        state_ref[0] = h
        state_ref[1] = u
        state_ref[2] = v
        high, low = split_two(h[PAD : PAD + cols])
        parts_ref[moment * cols : (moment + 1) * cols] = high
        parts_ref[spots + moment * cols : spots + (moment + 1) * cols] = low
    chunk = 512
    for start in range(0, nobs, chunk):
        here = slice(start, start + chunk)
        row, slot, col = rows_and_spots(cell_ref[:, here], slot_ref[:, here], cols)
        picked = dot(parts_ref[...], one_hot_rows(row, rows), NN)
        picked = picked[0:spots] + picked[spots : 2 * spots]
        spot_hot = lax.broadcasted_iota(jnp.int32, (spots, chunk), 0) == slot * cols + col
        out_ref[:, here] = jnp.sum(jnp.where(spot_hot, picked, 0.0), axis=0, keepdims=True)


def own_observed(inc, factors, cell, slot):
    _, cols, rows = inc.shape
    return call(
        forward_kernel,
        "forward",
        floats(1, cell.shape[1]),
        [
            pltpu.VMEM((3, cols + 2 * PAD, rows), F32),
            pltpu.VMEM((2 * STEPS * cols, rows), BF16),
        ],
        4 * 10**9,
    )(inc, factors, cell, slot)


def border_kernel(
    own_ref, west_ref, east_ref, factor_ref, cell_ref, slot_ref, out_ref, state_ref, parts_ref,
    *, cols,
):
    rows = west_ref.shape[1]
    nobs = cell_ref.shape[1]
    state_ref[...] = jnp.zeros(state_ref.shape, F32)
    for field in range(3):
        state_ref[field, PAD - HALO : PAD] = west_ref[edges_of(field)]
        state_ref[field, 3 * PAD : 3 * PAD + HALO] = east_ref[edges_of(field)]
    metric = factor_ref[0:1]
    coriolis = factor_ref[1:2]
    near = 2 * PAD
    spots = STEPS * near
    for moment in range(STEPS):
        h, u, v = model_step(state_ref[0], state_ref[1], state_ref[2], 1.0, metric, coriolis)
        state_ref[0] = h
        state_ref[1] = u
        state_ref[2] = v
        high, low = split_two(h[PAD : 3 * PAD])
        parts_ref[moment * near : (moment + 1) * near] = high
        parts_ref[spots + moment * near : spots + (moment + 1) * near] = low
    chunk = 512
    for start in range(0, nobs, chunk):
        here = slice(start, start + chunk)
        row, slot, col = rows_and_spots(cell_ref[:, here], slot_ref[:, here], cols)
        picked = dot(parts_ref[...], one_hot_rows(row, rows), NN)
        picked = picked[0:spots] + picked[spots : 2 * spots]
        east_spot = jnp.where(col >= cols - PAD, slot * near + (col - cols + near), -1)
        spot = jnp.where(col < PAD, slot * near + col, east_spot)
        spot_hot = lax.broadcasted_iota(jnp.int32, (spots, chunk), 0) == spot
        value = jnp.sum(jnp.where(spot_hot, picked, 0.0), axis=0, keepdims=True)
        value = value + own_ref[:, here]
        for i in range(0, chunk, 128):
            line = (start + i) // 128
            out_ref[:, line, :] = jnp.broadcast_to(value[:, i : i + 128], (out_ref.shape[0], 128))


def observed_parts(own, west, east, factors, cell, slot, cols, copies):
    rows = west.shape[1]
    return call(
        functools.partial(border_kernel, cols=cols),
        "border",
        floats(copies, cell.shape[1] // 128, 128),
        [
            pltpu.VMEM((3, 4 * PAD, rows), F32),
            pltpu.VMEM((4 * STEPS * PAD, rows), BF16),
        ],
        10**9,
    )(own, west, east, factors, cell, slot)


def adjoint_kernel(
    seen_ref, weight_ref, cell_ref, slot_ref, factor_ref, adj_ref, left_ref, right_ref,
    state_ref, force_ref,
):
    _, cols, rows = adj_ref.shape
    nobs = cell_ref.shape[1]
    spots = STEPS * cols
    chunk = 512
    seen = jnp.sum(seen_ref[...], axis=0)
    for start in range(0, nobs, chunk):
        here = slice(start, start + chunk)
        row, slot, col = rows_and_spots(cell_ref[:, here], slot_ref[:, here], cols)
        lines = range(start // 128, (start + chunk) // 128)
        total = jnp.concatenate([seen[i : i + 1] for i in lines], axis=1)
        weighted = weight_ref[:, here] * total
        spot_hot = lax.broadcasted_iota(jnp.int32, (spots, chunk), 0) == slot * cols + col
        high, low = split_two(jnp.where(spot_hot, weighted, 0.0))
        part = dot(jnp.concatenate([high, low], axis=0), one_hot_rows(row, rows), NT)
        part = part[0:spots] + part[spots : 2 * spots]
        if start == 0:
            force_ref[...] = part
        else:
            force_ref[...] += part
    metric = factor_ref[0:1]
    coriolis = factor_ref[1:2]
    state_ref[...] = jnp.zeros(state_ref.shape, F32)
    for moment in reversed(range(STEPS)):
        state_ref[0, PAD : PAD + cols] += force_ref[moment * cols : (moment + 1) * cols]
        h, u, v = model_step(state_ref[0], state_ref[1], state_ref[2], -1.0, metric, coriolis)
        state_ref[0] = h
        state_ref[1] = u
        state_ref[2] = v
    for field in range(3):
        adj_ref[field] = state_ref[field, PAD : PAD + cols]
        left_ref[edges_of(field)] = state_ref[field, PAD - HALO : PAD]
        right_ref[edges_of(field)] = state_ref[field, PAD + cols : PAD + cols + HALO]


def tile_adjoint(seen, weight, cell, slot, factors, cols):
    rows = factors.shape[1]
    return call(
        adjoint_kernel,
        "adjoint",
        [floats(3, cols, rows), floats(3 * HALO, rows), floats(3 * HALO, rows)],
        [
            pltpu.VMEM((3, cols + 2 * PAD, rows), F32),
            pltpu.VMEM((STEPS * cols, rows), F32),
        ],
        4 * 10**9,
    )(seen, weight, cell, slot, factors)


def three_products(parts_ref, high_ref, low_ref, lines):
    both = dot(parts_ref[...], high_ref[...], NN)
    rest = dot(parts_ref[0:lines], low_ref[...], NN)
    return both[0:lines] + both[lines : 2 * lines] + rest


def image_kernel(high_ref, low_ref, adj_ref, pert_ref, dir_ref, img_ref, parts_ref):
    members, cols, rows = dir_ref.shape
    lines = members * cols
    for m in range(members):
        projected = pert_ref[m, 0].astype(F32) * adj_ref[0]
        projected += pert_ref[m, 1].astype(F32) * adj_ref[1]
        projected += pert_ref[m, 2].astype(F32) * adj_ref[2]
        high, low = split_two(projected)
        parts_ref[m * cols : (m + 1) * cols] = high
        parts_ref[lines + m * cols : lines + (m + 1) * cols] = low
    pulled = three_products(parts_ref, high_ref, low_ref, lines)
    img_ref[...] = dir_ref[...] + pulled.reshape(members, cols, rows)


def own_image(high, low, adj, pert, direction):
    members, cols, rows = direction.shape
    return call(
        image_kernel,
        "image",
        floats(members, cols, rows),
        [pltpu.VMEM((2 * members * cols, rows), BF16)],
        10**9,
    )(high, low, adj, pert, direction)


def closing_kernel(
    high_ref, low_ref, own_ref, west_ref, east_ref, pert_ref, dir_ref, res_ref, img_ref, sums_ref,
    edge_ref, parts_ref,
):
    members, cols, rows = dir_ref.shape
    near = 2 * PAD
    lines = members * near
    edge_ref[...] = jnp.zeros(edge_ref.shape, F32)
    for field in range(3):
        edge_ref[field, 0:HALO] = west_ref[edges_of(field)]
        edge_ref[field, near - HALO : near] = east_ref[edges_of(field)]
    for m in range(members):
        west = jnp.zeros((PAD, rows), F32)
        east = jnp.zeros((PAD, rows), F32)
        for field in range(3):
            west += pert_ref[m, field, 0:PAD].astype(F32) * edge_ref[field, 0:PAD]
            east += pert_ref[m, field, cols - PAD : cols].astype(F32) * edge_ref[field, PAD:near]
        high, low = split_two(jnp.concatenate([west, east], axis=0))
        parts_ref[m * near : (m + 1) * near] = high
        parts_ref[lines + m * near : lines + (m + 1) * near] = low
    pulled = three_products(parts_ref, high_ref, low_ref, lines)
    totals = [jnp.zeros((8, rows), F32) for _ in range(4)]
    for m in range(members):
        for start in range(0, cols, PAD):
            here = slice(start, start + PAD)
            image = own_ref[m, here]
            if start == 0:
                image = image + pulled[m * near : m * near + PAD]
            if start == cols - PAD:
                image = image + pulled[m * near + PAD : (m + 1) * near]
            img_ref[m, here] = image
            way = dir_ref[m, here]
            left = res_ref[m, here]
            totals[0] += left * left
            totals[1] += way * image
            totals[2] += left * image
            totals[3] += image * image
    lane = lax.broadcasted_iota(jnp.int32, (1, 128), 1)
    packed = jnp.zeros((1, 128), F32)
    for i in range(4):
        total = jnp.sum(jnp.sum(totals[i], axis=0, keepdims=True), axis=1, keepdims=True)
        packed = jnp.where(lane == i, total, packed)
    sums_ref[...] = jnp.broadcast_to(packed, sums_ref.shape)


def image_and_sums(high, low, own, west, east, pert, direction, residual, copies):
    members, cols, rows = direction.shape
    return call(
        closing_kernel,
        "closing",
        [floats(members, cols, rows), floats(copies, 128)],
        [
            pltpu.VMEM((3, 2 * PAD, rows), F32),
            pltpu.VMEM((4 * members * PAD, rows), BF16),
        ],
        5 * 10**8,
    )(high, low, own, west, east, pert, direction, residual)


def update_kernel(
    sums_ref, control_ref, res_ref, dir_ref, img_ref, control_out, res_out, dir_out, new_ref, sems
):
    members, cols, rows = dir_ref.shape
    total = jnp.sum(sums_ref[...], axis=0, keepdims=True)
    lane = lax.broadcasted_iota(jnp.int32, (1, 128), 1)

    def lane_of(i):
        return jnp.sum(jnp.where(lane == i, total, 0.0), axis=1, keepdims=True)

    norm_old, curvature, cross_term, square = (lane_of(i) for i in range(4))
    step_size = norm_old / curvature
    norm_new = norm_old - 2.0 * step_size * cross_term + step_size * step_size * square
    ratio = norm_new / norm_old
    copies = []
    for m in range(members):
        way = dir_ref[m]
        left = res_ref[m] - step_size * img_ref[m]
        new_ref[0, m] = control_ref[m] + step_size * way
        new_ref[1, m] = left
        new_ref[2, m] = left + ratio * way
        for i, out in enumerate((control_out, res_out, dir_out)):
            copy = pltpu.make_async_copy(new_ref.at[i, m], out.at[m], sems.at[3 * m + i])
            copy.start()
            copies.append(copy)
    for copy in copies:
        copy.wait()


def updated(sums, control, residual, direction, image):
    members = control.shape[0]
    return call(
        update_kernel,
        "update",
        [floats(*control.shape)] * 3,
        [pltpu.VMEM((3, *control.shape), F32), pltpu.SemaphoreType.DMA((3 * members,))],
        10**7,
        out_specs=[HBM, HBM, HBM],
    )(sums, control, residual, direction, image)


def neighbours(to_west, to_east):
    count = lax.axis_size(LON)
    east = [(i, (i + 1) % count) for i in range(count)]
    west = [(target, source) for source, target in east]
    from_west = lax.ppermute(to_east, LON, east)
    from_east = lax.ppermute(to_west, LON, west)
    return from_west, from_east


def body(control, residual, direction, ens_perturb, localize, obs_cell, obs_slot, obs_weight):
    cols = control.shape[2]
    factors = jnp.asarray(grid_factors(localize.shape[0]))
    turned = lambda x: jnp.swapaxes(x, 1, 2)
    control_t, residual_t, direction_t = turned(control), turned(residual), turned(direction)
    pert = jnp.swapaxes(ens_perturb, 2, 3)
    cell, slot, weight = obs_cell[None], obs_slot[None], obs_weight[None]
    inc, left, right, high, low = partial_increment(localize, direction_t, pert)
    west, east = neighbours(left, right)
    own = own_observed(inc, factors, cell, slot)
    seen = observed_parts(own, west, east, factors, cell, slot, cols, lax.axis_size(ENS))
    seen = lax.all_to_all(seen, ENS, 0, 0, tiled=True)
    adj, left, right = tile_adjoint(seen, weight, cell, slot, factors, cols)
    west, east = neighbours(left, right)
    image = own_image(high, low, adj, pert, direction_t)
    image, sums = image_and_sums(
        high, low, image, west, east, pert, direction_t, residual_t, lax.axis_size(ENS_LON)
    )
    sums = lax.all_to_all(sums, ENS_LON, 0, 0, tiled=True)
    results = updated(sums, control_t, residual_t, direction_t, image)
    return tuple(turned(x) for x in results)


def solution(mesh):
    split = Mesh(mesh.devices.reshape(2, 4, 8, 2, 2), ("ens_0", "ens_1", "lon_0", "lon_1", "lon_2"))
    placed = (
        P(ENS, None, LON),
        P(ENS, None, LON),
        P(ENS, None, LON),
        P(ENS, None, None, LON),
        P(),
        P(LON),
        P(LON),
        P(LON),
    )
    return jax.shard_map(
        body,
        mesh=split,
        in_specs=placed,
        out_specs=(P(ENS, None, LON), P(ENS, None, LON), P(ENS, None, LON)),
        check_vma=False,
    )
```

```python
import jax
import jax.numpy as jnp
import numpy as np
from jax import lax
from jax.experimental import pallas as pl
from jax.experimental.pallas import tpu as pltpu
from jax.sharding import Mesh
from jax.sharding import PartitionSpec as P

STEPS = 3
HALO = 3
PAD = 8
LON = ("lon_0", "lon_1", "lon_2")
ENS = ("ens_0", "ens_1")
ENS_LON = ("ens_0", "ens_1", "lon_0", "lon_1", "lon_2")

wave_speed = 0.35
rotation = 0.2

F32 = jnp.float32
BF16 = jnp.bfloat16
NT = (((1,), (1,)), ((), ()))
NN = (((1,), (0,)), ((), ()))
HBM = pl.BlockSpec(memory_space=pltpu.HBM)


def split_two(x):
    high = x.astype(BF16)
    low = (x - high.astype(F32)).astype(BF16)
    return high, low


def dot(a, b, dims):
    return lax.dot_general(a, b, dims, preferred_element_type=F32)


def grid_factors(lat_total):
    row_ids = np.arange(lat_total).astype(np.float32)
    latitude = (-1.0 / 3.0 + 2.0 / 3.0 * (row_ids + 0.5) / lat_total) * np.pi
    return np.stack([1.0 / np.cos(latitude), np.sin(latitude)]).astype(np.float32)


def model_step(h, u, v, orient, metric, coriolis):
    wide, rows = h.shape
    lane = lax.broadcasted_iota(jnp.int32, (1, rows), 1)
    lon_scale = (orient * wave_speed * 0.5) * metric
    lat_scale = orient * wave_speed * 0.5
    turn = (orient * rotation) * coriolis
    keep_next = jnp.where(lane == rows - 1, 0.0, lat_scale)
    keep_last = jnp.where(lane == 0, 0.0, lat_scale)

    def lon_diff(x):
        return lon_scale * (pltpu.roll(x, wide - 1, 0) - pltpu.roll(x, 1, 0))

    def lat_diff(x):
        return keep_next * pltpu.roll(x, rows - 1, 1) - keep_last * pltpu.roll(x, 1, 1)

    return (
        h - (lon_diff(u) + lat_diff(v)),
        u - lon_diff(h) + turn * v,
        v - lat_diff(h) - turn * u,
    )


def call(kernel, name, out_shape, scratch, flops, limit_mib=24, **options):
    return pl.pallas_call(
        kernel,
        name=name,
        out_shape=out_shape,
        scratch_shapes=scratch,
        compiler_params=pltpu.CompilerParams(vmem_limit_bytes=limit_mib << 20),
        cost_estimate=pl.CostEstimate(flops=flops, bytes_accessed=1 << 20, transcendentals=0),
        **options,
    )


def floats(*dims):
    return jax.ShapeDtypeStruct(dims, F32)


def rows_and_spots(cell, slot, cols):
    bits = cols.bit_length() - 1
    assert cols == 1 << bits
    return lax.shift_right_logical(cell, bits), slot, cell & (cols - 1)


def one_hot_rows(row, rows):
    ids = lax.broadcasted_iota(jnp.int16, (rows, row.shape[1]), 0)
    return jnp.where(ids == row.astype(jnp.int16), jnp.ones((), BF16), jnp.zeros((), BF16))


def on_odd_tile():
    return lax.axis_index("lon_2") == 1


def edges_of(field):
    return slice(HALO * field, HALO * (field + 1))


def increment_kernel(
    loc_hbm, dir_hbm, pert_hbm, inc_ref, inner_ref, outer_ref, high_ref, low_ref,
    loc_ref, dir_ref, pert_ref, parts_ref, sems,
):
    members, cols, rows = dir_ref.shape
    lines = members * cols
    block = 256
    blocks = rows // block
    first = pltpu.make_async_copy(dir_hbm, dir_ref, sems.at[0])
    second = pltpu.make_async_copy(pert_hbm, pert_ref, sems.at[1])
    places = [slice(i * block, (i + 1) * block) for i in range(blocks)]
    copies = [
        pltpu.make_async_copy(loc_hbm.at[here], loc_ref.at[here], sems.at[2 + i])
        for i, here in enumerate(places)
    ]
    odd = on_odd_tile()
    first.start()
    copies[0].start()
    copies[1].start()
    first.wait()
    copies[2].start()
    high, low = split_two(dir_ref[...].reshape(lines, rows))
    parts_ref[0:lines] = high
    parts_ref[lines : 2 * lines] = low
    for i in range(blocks + 1):
        if i < blocks:
            copies[i].wait()
            if i == 0:
                second.start()
                for copy in copies[3:]:
                    copy.start()
            high_ref[places[i]], low_ref[places[i]] = split_two(loc_ref[places[i]])
        if i == 0:
            continue
        if i == 1:
            second.wait()
        here = places[i - 1]
        both = dot(parts_ref[...], high_ref[here], NT)
        rest = dot(parts_ref[0:lines], low_ref[here], NT)
        localized = both[0:lines] + both[lines : 2 * lines] + rest
        for field in range(3):
            total = None
            for m in range(members):
                term = pert_ref[m, field, :, here].astype(F32) * localized[m * cols : (m + 1) * cols]
                total = term if total is None else total + term
            inc_ref[field, :, here] = total
            west, east = total[0:HALO], total[cols - HALO : cols]
            inner_ref[edges_of(field), here] = jnp.where(odd, west, east)
            outer_ref[edges_of(field), here] = jnp.where(odd, east, west)


def partial_increment(localize, direction, pert):
    members, cols, rows = direction.shape
    half = jax.ShapeDtypeStruct((rows, rows), BF16)
    return call(
        increment_kernel,
        "increment",
        [floats(3, cols, rows), floats(3 * HALO, rows), floats(3 * HALO, rows), half, half],
        [
            pltpu.VMEM((rows, rows), F32),
            pltpu.VMEM(direction.shape, F32),
            pltpu.VMEM(pert.shape, BF16),
            pltpu.VMEM((2 * members * cols, rows), BF16),
            pltpu.SemaphoreType.DMA((2 + rows // 256,)),
        ],
        10**9,
        in_specs=[HBM, HBM, HBM],
    )(*(pltpu.with_memory_space_constraint(x, pltpu.HBM) for x in (localize, direction, pert)))


def forward_steps(state_ref, factor_ref, parts_ref, places):
    metric = factor_ref[0:1]
    coriolis = factor_ref[1:2]
    count = sum(stop - start for start, stop in places)
    for moment in range(STEPS):
        h, u, v = model_step(state_ref[0], state_ref[1], state_ref[2], 1.0, metric, coriolis)
        if moment + 1 < STEPS:
            state_ref[0] = h
            state_ref[1] = u
            state_ref[2] = v
        line = moment * count
        for start, stop in places:
            high, low = split_two(h[start:stop])
            parts_ref[line : line + stop - start] = high
            parts_ref[STEPS * count + line : STEPS * count + line + stop - start] = low
            line += stop - start


def sampled(parts_ref, row, spot, rows):
    spots = parts_ref.shape[0] // 2
    picked = dot(parts_ref[...], one_hot_rows(row, rows), NN)
    picked = picked[0:spots] + picked[spots : 2 * spots]
    spot_hot = lax.broadcasted_iota(jnp.int32, picked.shape, 0) == spot
    return jnp.sum(jnp.where(spot_hot, picked, 0.0), axis=0, keepdims=True)


def forward_kernel(inc_ref, factor_ref, cell_ref, slot_ref, out_ref, state_ref, parts_ref):
    _, cols, rows = inc_ref.shape
    nobs = cell_ref.shape[1]
    state_ref[...] = inc_ref[...]
    forward_steps(state_ref, factor_ref, parts_ref, ((PAD, cols - PAD),))
    chunk = 512
    for start in range(0, nobs, chunk):
        here = slice(start, start + chunk)
        row, slot, col = rows_and_spots(cell_ref[:, here], slot_ref[:, here], cols)
        within = (col >= PAD) & (col < cols - PAD)
        spot = jnp.where(within, slot * (cols - 2 * PAD) + (col - PAD), -1)
        out_ref[:, here] = sampled(parts_ref, row, spot, rows)


def inner_observed(inc, factors, cell, slot):
    _, cols, rows = inc.shape
    return call(
        forward_kernel,
        "forward",
        floats(1, cell.shape[1]),
        [
            pltpu.VMEM((3, cols, rows), F32),
            pltpu.VMEM((2 * STEPS * (cols - 2 * PAD), rows), BF16),
        ],
        4 * 10**9,
    )(inc, factors, cell, slot)


def border_kernel(
    seen_ref, inc_ref, inner_ref, outer_ref, factor_ref, cell_ref, slot_ref, out_ref,
    state_ref, parts_ref,
):
    _, cols, rows = inc_ref.shape
    nobs = cell_ref.shape[1]
    odd = on_odd_tile()
    state_ref[...] = jnp.zeros(state_ref.shape, F32)
    for field in range(3):
        inner, outer = inner_ref[edges_of(field)], outer_ref[edges_of(field)]
        state_ref[field, PAD - HALO : PAD] = jnp.where(odd, inner, outer)
        state_ref[field, PAD : 3 * PAD] = inc_ref[field, 0 : 2 * PAD]
        state_ref[field, 3 * PAD : 5 * PAD] = inc_ref[field, cols - 2 * PAD : cols]
        state_ref[field, 5 * PAD : 5 * PAD + HALO] = jnp.where(odd, outer, inner)
    forward_steps(state_ref, factor_ref, parts_ref, ((PAD, 2 * PAD), (4 * PAD, 5 * PAD)))
    near = 2 * PAD
    chunk = 512
    for start in range(0, nobs, chunk):
        here = slice(start, start + chunk)
        row, slot, col = rows_and_spots(cell_ref[:, here], slot_ref[:, here], cols)
        east_spot = jnp.where(col >= cols - PAD, slot * near + (col - cols + near), -1)
        spot = jnp.where(col < PAD, slot * near + col, east_spot)
        value = sampled(parts_ref, row, spot, rows) + seen_ref[:, here]
        for i in range(0, chunk, 128):
            line = (start + i) // 128
            out_ref[:, line, :] = jnp.broadcast_to(value[:, i : i + 128], (out_ref.shape[0], 128))


def observed_parts(seen, inc, inner, outer, factors, cell, slot, copies):
    rows = inc.shape[2]
    return call(
        border_kernel,
        "border",
        floats(copies, cell.shape[1] // 128, 128),
        [
            pltpu.VMEM((3, 6 * PAD, rows), F32),
            pltpu.VMEM((4 * STEPS * PAD, rows), BF16),
        ],
        10**9,
    )(seen, inc, inner, outer, factors, cell, slot)


def adjoint_kernel(
    seen_ref, weight_ref, cell_ref, slot_ref, factor_ref, adj_ref, inner_ref, outer_ref,
    state_ref, force_ref,
):
    _, cols, rows = adj_ref.shape
    nobs = cell_ref.shape[1]
    spots = STEPS * cols
    chunk = 512
    seen = jnp.sum(seen_ref[...], axis=0)
    for start in range(0, nobs, chunk):
        here = slice(start, start + chunk)
        row, slot, col = rows_and_spots(cell_ref[:, here], slot_ref[:, here], cols)
        lines = range(start // 128, (start + chunk) // 128)
        total = jnp.concatenate([seen[i : i + 1] for i in lines], axis=1)
        weighted = weight_ref[:, here] * total
        spot_hot = lax.broadcasted_iota(jnp.int32, (spots, chunk), 0) == slot * cols + col
        high, low = split_two(jnp.where(spot_hot, weighted, 0.0))
        part = dot(jnp.concatenate([high, low], axis=0), one_hot_rows(row, rows), NT)
        part = part[0:spots] + part[spots : 2 * spots]
        if start == 0:
            force_ref[...] = part
        else:
            force_ref[...] += part
    metric = factor_ref[0:1]
    coriolis = factor_ref[1:2]
    state_ref[...] = jnp.zeros(state_ref.shape, F32)
    for moment in reversed(range(STEPS)):
        state_ref[0, PAD : PAD + cols] += force_ref[moment * cols : (moment + 1) * cols]
        h, u, v = model_step(state_ref[0], state_ref[1], state_ref[2], -1.0, metric, coriolis)
        state_ref[0] = h
        state_ref[1] = u
        state_ref[2] = v
    odd = on_odd_tile()
    for field in range(3):
        adj_ref[field] = state_ref[field, PAD : PAD + cols]
        west = state_ref[field, PAD - HALO : PAD]
        east = state_ref[field, PAD + cols : PAD + cols + HALO]
        inner_ref[edges_of(field)] = jnp.where(odd, west, east)
        outer_ref[edges_of(field)] = jnp.where(odd, east, west)


def tile_adjoint(seen, weight, cell, slot, factors, cols):
    rows = factors.shape[1]
    return call(
        adjoint_kernel,
        "adjoint",
        [floats(3, cols, rows), floats(3 * HALO, rows), floats(3 * HALO, rows)],
        [
            pltpu.VMEM((3, cols + 2 * PAD, rows), F32),
            pltpu.VMEM((STEPS * cols, rows), F32),
        ],
        4 * 10**9,
    )(seen, weight, cell, slot, factors)


def three_products(parts_ref, high_ref, low_ref, lines):
    both = dot(parts_ref[...], high_ref[...], NN)
    rest = dot(parts_ref[0:lines], low_ref[...], NN)
    return both[0:lines] + both[lines : 2 * lines] + rest


def image_kernel(high_ref, low_ref, adj_ref, pert_ref, dir_ref, img_ref, parts_ref):
    members, cols, rows = dir_ref.shape
    lines = members * cols
    for m in range(members):
        projected = pert_ref[m, 0].astype(F32) * adj_ref[0]
        projected += pert_ref[m, 1].astype(F32) * adj_ref[1]
        projected += pert_ref[m, 2].astype(F32) * adj_ref[2]
        high, low = split_two(projected)
        parts_ref[m * cols : (m + 1) * cols] = high
        parts_ref[lines + m * cols : lines + (m + 1) * cols] = low
    pulled = three_products(parts_ref, high_ref, low_ref, lines)
    img_ref[...] = dir_ref[...] + pulled.reshape(members, cols, rows)


def own_image(high, low, adj, pert, direction):
    members, cols, rows = direction.shape
    return call(
        image_kernel,
        "image",
        floats(members, cols, rows),
        [pltpu.VMEM((2 * members * cols, rows), BF16)],
        10**9,
    )(high, low, adj, pert, direction)


def closing_kernel(
    high_ref, low_ref, own_ref, inner_ref, outer_ref, pert_ref, dir_ref, res_ref, img_ref, sums_ref,
    edge_ref, parts_ref,
):
    members, cols, rows = dir_ref.shape
    near = 2 * PAD
    lines = members * near
    odd = on_odd_tile()
    edge_ref[...] = jnp.zeros(edge_ref.shape, F32)
    for field in range(3):
        inner, outer = inner_ref[edges_of(field)], outer_ref[edges_of(field)]
        edge_ref[field, 0:HALO] = jnp.where(odd, inner, outer)
        edge_ref[field, near - HALO : near] = jnp.where(odd, outer, inner)
    for m in range(members):
        west = jnp.zeros((PAD, rows), F32)
        east = jnp.zeros((PAD, rows), F32)
        for field in range(3):
            west += pert_ref[m, field, 0:PAD].astype(F32) * edge_ref[field, 0:PAD]
            east += pert_ref[m, field, cols - PAD : cols].astype(F32) * edge_ref[field, PAD:near]
        high, low = split_two(jnp.concatenate([west, east], axis=0))
        parts_ref[m * near : (m + 1) * near] = high
        parts_ref[lines + m * near : lines + (m + 1) * near] = low
    pulled = three_products(parts_ref, high_ref, low_ref, lines)
    totals = [jnp.zeros((8, rows), F32) for _ in range(4)]
    for m in range(members):
        for start in range(0, cols, PAD):
            here = slice(start, start + PAD)
            image = own_ref[m, here]
            if start == 0:
                image = image + pulled[m * near : m * near + PAD]
            if start == cols - PAD:
                image = image + pulled[m * near + PAD : (m + 1) * near]
            img_ref[m, here] = image
            way = dir_ref[m, here]
            left = res_ref[m, here]
            totals[0] += left * left
            totals[1] += way * image
            totals[2] += left * image
            totals[3] += image * image
    lane = lax.broadcasted_iota(jnp.int32, (1, 128), 1)
    packed = jnp.zeros((1, 128), F32)
    for i in range(4):
        total = jnp.sum(jnp.sum(totals[i], axis=0, keepdims=True), axis=1, keepdims=True)
        packed = jnp.where(lane == i, total, packed)
    sums_ref[...] = jnp.broadcast_to(packed, sums_ref.shape)


def image_and_sums(high, low, own, inner, outer, pert, direction, residual, copies):
    members, cols, rows = direction.shape
    return call(
        closing_kernel,
        "closing",
        [floats(members, cols, rows), floats(copies, 128)],
        [
            pltpu.VMEM((3, 2 * PAD, rows), F32),
            pltpu.VMEM((4 * members * PAD, rows), BF16),
        ],
        5 * 10**8,
    )(high, low, own, inner, outer, pert, direction, residual)


def update_kernel(
    sums_ref, control_ref, res_ref, dir_ref, img_ref, control_out, res_out, dir_out, new_ref, sems
):
    members, cols, rows = dir_ref.shape
    total = jnp.sum(sums_ref[...], axis=0, keepdims=True)
    lane = lax.broadcasted_iota(jnp.int32, (1, 128), 1)

    def lane_of(i):
        return jnp.sum(jnp.where(lane == i, total, 0.0), axis=1, keepdims=True)

    norm_old, curvature, cross_term, square = (lane_of(i) for i in range(4))
    step_size = norm_old / curvature
    norm_new = norm_old - 2.0 * step_size * cross_term + step_size * step_size * square
    ratio = norm_new / norm_old
    copies = []
    for m in range(members):
        way = dir_ref[m]
        left = res_ref[m] - step_size * img_ref[m]
        new_ref[0, m] = control_ref[m] + step_size * way
        new_ref[1, m] = left
        new_ref[2, m] = left + ratio * way
        for i, out in enumerate((control_out, res_out, dir_out)):
            copy = pltpu.make_async_copy(new_ref.at[i, m], out.at[m], sems.at[3 * m + i])
            copy.start()
            copies.append(copy)
    for copy in copies:
        copy.wait()


def updated(sums, control, residual, direction, image):
    members = control.shape[0]
    return call(
        update_kernel,
        "update",
        [floats(*control.shape)] * 3,
        [pltpu.VMEM((3, *control.shape), F32), pltpu.SemaphoreType.DMA((3 * members,))],
        10**7,
        out_specs=[HBM, HBM, HBM],
    )(sums, control, residual, direction, image)


def swapped(inner, outer):
    count = lax.axis_size(LON)
    inner_pairs = [(i, i ^ 1) for i in range(count)]
    outer_pairs = [(i, ((i + 1) ^ 1) - 1) for i in range(count)]
    outer_pairs = [(source, target % count) for source, target in outer_pairs]
    return lax.ppermute(inner, LON, inner_pairs), lax.ppermute(outer, LON, outer_pairs)


def body(control, residual, direction, ens_perturb, localize, obs_cell, obs_slot, obs_weight):
    cols = control.shape[2]
    factors = jnp.asarray(grid_factors(localize.shape[0]))
    turned = lambda x: jnp.swapaxes(x, 1, 2)
    control_t, residual_t, direction_t = turned(control), turned(residual), turned(direction)
    pert = jnp.swapaxes(ens_perturb, 2, 3)
    cell, slot, weight = obs_cell[None], obs_slot[None], obs_weight[None]
    inc, inner, outer, high, low = partial_increment(localize, direction_t, pert)
    inner, outer = swapped(inner, outer)
    seen = inner_observed(inc, factors, cell, slot)
    seen = observed_parts(seen, inc, inner, outer, factors, cell, slot, lax.axis_size(ENS))
    seen = lax.all_to_all(seen, ENS, 0, 0, tiled=True)
    adj, inner, outer = tile_adjoint(seen, weight, cell, slot, factors, cols)
    inner, outer = swapped(inner, outer)
    image = own_image(high, low, adj, pert, direction_t)
    image, sums = image_and_sums(
        high, low, image, inner, outer, pert, direction_t, residual_t, lax.axis_size(ENS_LON)
    )
    sums = lax.all_to_all(sums, ENS_LON, 0, 0, tiled=True)
    results = updated(sums, control_t, residual_t, direction_t, image)
    return tuple(turned(x) for x in results)


def solution(mesh):
    split = Mesh(mesh.devices.reshape(2, 4, 8, 2, 2), ("ens_0", "ens_1", "lon_0", "lon_1", "lon_2"))
    placed = (
        P(ENS, None, LON),
        P(ENS, None, LON),
        P(ENS, None, LON),
        P(ENS, None, None, LON),
        P(),
        P(LON),
        P(LON),
        P(LON),
    )
    return jax.shard_map(
        body,
        mesh=split,
        in_specs=placed,
        out_specs=(P(ENS, None, LON), P(ENS, None, LON), P(ENS, None, LON)),
        check_vma=False,
    )
```

```python
import jax
import jax.numpy as jnp
import numpy as np
from jax import lax
from jax.experimental import pallas as pl
from jax.experimental.pallas import tpu as pltpu
from jax.sharding import Mesh
from jax.sharding import PartitionSpec as P

STEPS = 3
HALO = 3
PAD = 8
LON = ("lon_0", "lon_1", "lon_2")
ENS = ("ens_0", "ens_1")
ENS_LON = ("ens_0", "ens_1", "lon_0", "lon_1", "lon_2")

wave_speed = 0.35
rotation = 0.2

F32 = jnp.float32
BF16 = jnp.bfloat16
NT = (((1,), (1,)), ((), ()))
NN = (((1,), (0,)), ((), ()))
HBM = pl.BlockSpec(memory_space=pltpu.HBM)


def split_two(x):
    high = x.astype(BF16)
    low = (x - high.astype(F32)).astype(BF16)
    return high, low


def dot(a, b, dims):
    return lax.dot_general(a, b, dims, preferred_element_type=F32)


def grid_factors(lat_total):
    row_ids = np.arange(lat_total).astype(np.float32)
    latitude = (-1.0 / 3.0 + 2.0 / 3.0 * (row_ids + 0.5) / lat_total) * np.pi
    return np.stack([1.0 / np.cos(latitude), np.sin(latitude)]).astype(np.float32)


def model_step(h, u, v, orient, metric, coriolis):
    wide, rows = h.shape
    lane = lax.broadcasted_iota(jnp.int32, (1, rows), 1)
    lon_scale = (orient * wave_speed * 0.5) * metric
    lat_scale = orient * wave_speed * 0.5
    turn = (orient * rotation) * coriolis
    keep_next = jnp.where(lane == rows - 1, 0.0, lat_scale)
    keep_last = jnp.where(lane == 0, 0.0, lat_scale)

    def lon_diff(x):
        return lon_scale * (pltpu.roll(x, wide - 1, 0) - pltpu.roll(x, 1, 0))

    def lat_diff(x):
        return keep_next * pltpu.roll(x, rows - 1, 1) - keep_last * pltpu.roll(x, 1, 1)

    return (
        h - (lon_diff(u) + lat_diff(v)),
        u - lon_diff(h) + turn * v,
        v - lat_diff(h) - turn * u,
    )


def call(kernel, name, out_shape, scratch, flops, limit_mib=24, **options):
    return pl.pallas_call(
        kernel,
        name=name,
        out_shape=out_shape,
        scratch_shapes=scratch,
        compiler_params=pltpu.CompilerParams(vmem_limit_bytes=limit_mib << 20),
        cost_estimate=pl.CostEstimate(flops=flops, bytes_accessed=1 << 20, transcendentals=0),
        **options,
    )


def floats(*dims):
    return jax.ShapeDtypeStruct(dims, F32)


def rows_and_spots(cell, slot, cols):
    bits = cols.bit_length() - 1
    assert cols == 1 << bits
    return lax.shift_right_logical(cell, bits), slot, cell & (cols - 1)


def one_hot_rows(row, rows):
    ids = lax.broadcasted_iota(jnp.int16, (rows, row.shape[1]), 0)
    return jnp.where(ids == row.astype(jnp.int16), jnp.ones((), BF16), jnp.zeros((), BF16))


def on_odd_tile():
    return lax.axis_index("lon_2") == 1


def put_edge(ref, field, lanes, value):
    for i in range(lanes // 128, lanes // 128 + value.shape[1] // 128):
        line = 3 * HALO * i + HALO * field
        at = i * 128 - lanes
        ref[line : line + HALO] = value[:, at : at + 128]


def get_edge(ref, field):
    tiles = range(ref.shape[0] // (3 * HALO))
    lines = [3 * HALO * i + HALO * field for i in tiles]
    return jnp.concatenate([ref[line : line + HALO] for line in lines], axis=1)


def edge_floats(rows):
    return floats(3 * HALO * rows // 128, 128)


def increment_kernel(
    loc_hbm, dir_hbm, pert_hbm, inc_ref, inner_ref, outer_ref, high_ref, low_ref,
    loc_ref, dir_ref, pert_ref, parts_ref, sems,
):
    members, cols, rows = dir_ref.shape
    lines = members * cols
    block = 256
    blocks = rows // block
    first = pltpu.make_async_copy(dir_hbm, dir_ref, sems.at[0])
    second = pltpu.make_async_copy(pert_hbm, pert_ref, sems.at[1])
    places = [slice(i * block, (i + 1) * block) for i in range(blocks)]
    copies = [
        pltpu.make_async_copy(loc_hbm.at[here], loc_ref.at[here], sems.at[2 + i])
        for i, here in enumerate(places)
    ]
    odd = on_odd_tile()
    first.start()
    copies[0].start()
    second.start()
    for copy in copies[1:]:
        copy.start()
    first.wait()
    high, low = split_two(dir_ref[...].reshape(lines, rows))
    parts_ref[0:lines] = high
    parts_ref[lines : 2 * lines] = low
    for i in range(blocks + 1):
        if i < blocks:
            copies[i].wait()
            high_ref[places[i]], low_ref[places[i]] = split_two(loc_ref[places[i]])
        if i == 0:
            continue
        if i == 1:
            second.wait()
        here = places[i - 1]
        both = dot(parts_ref[...], high_ref[here], NT)
        rest = dot(parts_ref[0:lines], low_ref[here], NT)
        localized = both[0:lines] + both[lines : 2 * lines] + rest
        for field in range(3):
            total = None
            for m in range(members):
                term = pert_ref[m, field, :, here].astype(F32) * localized[m * cols : (m + 1) * cols]
                total = term if total is None else total + term
            inc_ref[field, :, here] = total
            west, east = total[0:HALO], total[cols - HALO : cols]
            put_edge(inner_ref, field, here.start, jnp.where(odd, west, east))
            put_edge(outer_ref, field, here.start, jnp.where(odd, east, west))


def partial_increment(localize, direction, pert):
    members, cols, rows = direction.shape
    half = jax.ShapeDtypeStruct((rows, rows), BF16)
    return call(
        increment_kernel,
        "increment",
        [floats(3, cols, rows), edge_floats(rows), edge_floats(rows), half, half],
        [
            pltpu.VMEM((rows, rows), F32),
            pltpu.VMEM(direction.shape, F32),
            pltpu.VMEM(pert.shape, BF16),
            pltpu.VMEM((2 * members * cols, rows), BF16),
            pltpu.SemaphoreType.DMA((2 + rows // 256,)),
        ],
        10**9,
        in_specs=[HBM, HBM, HBM],
    )(*(pltpu.with_memory_space_constraint(x, pltpu.HBM) for x in (localize, direction, pert)))


def forward_steps(state_ref, factor_ref, parts_ref, places):
    metric = factor_ref[0:1]
    coriolis = factor_ref[1:2]
    count = sum(stop - start for start, stop in places)
    for moment in range(STEPS):
        h, u, v = model_step(state_ref[0], state_ref[1], state_ref[2], 1.0, metric, coriolis)
        if moment + 1 < STEPS:
            state_ref[0] = h
            state_ref[1] = u
            state_ref[2] = v
        line = moment * count
        for start, stop in places:
            high, low = split_two(h[start:stop])
            parts_ref[line : line + stop - start] = high
            parts_ref[STEPS * count + line : STEPS * count + line + stop - start] = low
            line += stop - start


def sampled(parts_ref, row, spot, rows):
    spots = parts_ref.shape[0] // 2
    picked = dot(parts_ref[...], one_hot_rows(row, rows), NN)
    picked = picked[0:spots] + picked[spots : 2 * spots]
    spot_hot = lax.broadcasted_iota(jnp.int32, picked.shape, 0) == spot
    return jnp.sum(jnp.where(spot_hot, picked, 0.0), axis=0, keepdims=True)


def forward_kernel(inc_ref, factor_ref, cell_ref, slot_ref, out_ref, state_ref, parts_ref):
    _, cols, rows = inc_ref.shape
    nobs = cell_ref.shape[1]
    state_ref[...] = inc_ref[...]
    forward_steps(state_ref, factor_ref, parts_ref, ((PAD, cols - PAD),))
    chunk = 512
    for start in range(0, nobs, chunk):
        here = slice(start, start + chunk)
        row, slot, col = rows_and_spots(cell_ref[:, here], slot_ref[:, here], cols)
        within = (col >= PAD) & (col < cols - PAD)
        spot = jnp.where(within, slot * (cols - 2 * PAD) + (col - PAD), -1)
        out_ref[:, here] = sampled(parts_ref, row, spot, rows)


def inner_observed(inc, factors, cell, slot):
    _, cols, rows = inc.shape
    return call(
        forward_kernel,
        "forward",
        floats(1, cell.shape[1]),
        [
            pltpu.VMEM((3, cols, rows), F32),
            pltpu.VMEM((2 * STEPS * (cols - 2 * PAD), rows), BF16),
        ],
        4 * 10**9,
    )(inc, factors, cell, slot)


def border_kernel(
    seen_ref, inc_ref, inner_ref, outer_ref, factor_ref, cell_ref, slot_ref, out_ref,
    state_ref, parts_ref,
):
    _, cols, rows = inc_ref.shape
    nobs = cell_ref.shape[1]
    odd = on_odd_tile()
    state_ref[...] = jnp.zeros(state_ref.shape, F32)
    for field in range(3):
        inner, outer = get_edge(inner_ref, field), get_edge(outer_ref, field)
        state_ref[field, PAD - HALO : PAD] = jnp.where(odd, inner, outer)
        state_ref[field, PAD : 3 * PAD] = inc_ref[field, 0 : 2 * PAD]
        state_ref[field, 3 * PAD : 5 * PAD] = inc_ref[field, cols - 2 * PAD : cols]
        state_ref[field, 5 * PAD : 5 * PAD + HALO] = jnp.where(odd, outer, inner)
    forward_steps(state_ref, factor_ref, parts_ref, ((PAD, 2 * PAD), (4 * PAD, 5 * PAD)))
    near = 2 * PAD
    chunk = 512
    for start in range(0, nobs, chunk):
        here = slice(start, start + chunk)
        row, slot, col = rows_and_spots(cell_ref[:, here], slot_ref[:, here], cols)
        east_spot = jnp.where(col >= cols - PAD, slot * near + (col - cols + near), -1)
        spot = jnp.where(col < PAD, slot * near + col, east_spot)
        value = sampled(parts_ref, row, spot, rows) + seen_ref[:, here]
        for i in range(0, chunk, 128):
            line = (start + i) // 128
            out_ref[:, line, :] = jnp.broadcast_to(value[:, i : i + 128], (out_ref.shape[0], 128))


def observed_parts(seen, inc, inner, outer, factors, cell, slot, copies):
    rows = inc.shape[2]
    return call(
        border_kernel,
        "border",
        floats(copies, cell.shape[1] // 128, 128),
        [
            pltpu.VMEM((3, 6 * PAD, rows), F32),
            pltpu.VMEM((4 * STEPS * PAD, rows), BF16),
        ],
        10**9,
    )(seen, inc, inner, outer, factors, cell, slot)


def backward_steps(state_ref, factor_ref, add_force):
    metric = factor_ref[0:1]
    coriolis = factor_ref[1:2]
    state_ref[...] = jnp.zeros(state_ref.shape, F32)
    for moment in reversed(range(STEPS)):
        add_force(moment)
        h, u, v = model_step(state_ref[0], state_ref[1], state_ref[2], -1.0, metric, coriolis)
        state_ref[0] = h
        state_ref[1] = u
        state_ref[2] = v


def placed(spots, spot, weighted):
    spot_hot = lax.broadcasted_iota(jnp.int32, (spots, spot.shape[1]), 0) == spot
    return jnp.concatenate(split_two(jnp.where(spot_hot, weighted, 0.0)), axis=0)


def gather_force(force_ref, part, start):
    spots = force_ref.shape[0]
    part = part[0:spots] + part[spots : 2 * spots]
    if start == 0:
        force_ref[...] = part
    else:
        force_ref[...] += part


def edge_adjoint_kernel(
    seen_ref, weight_ref, cell_ref, slot_ref, lines_ref, factor_ref,
    weighted_ref, force_ref, inner_ref, outer_ref, state_ref, *, cols,
):
    rows = factor_ref.shape[1]
    nobs = cell_ref.shape[1]
    near = 2 * PAD
    chunk = 512
    seen = jnp.sum(seen_ref[...], axis=0)
    upright = jnp.transpose(lax.shift_right_logical(lines_ref[...], cols.bit_length() - 1))
    ids = lax.broadcasted_iota(jnp.int16, (128, rows), 1)
    for start in range(0, nobs, chunk):
        here = slice(start, start + chunk)
        _, slot, col = rows_and_spots(cell_ref[:, here], slot_ref[:, here], cols)
        lines = range(start // 128, (start + chunk) // 128)
        weighted = weight_ref[:, here] * jnp.concatenate([seen[i : i + 1] for i in lines], axis=1)
        weighted_ref[:, here] = weighted
        east_spot = jnp.where(col >= cols - PAD, slot * near + (col - cols + near), -1)
        spot = jnp.where(col < PAD, slot * near + col, east_spot)
        hots = []
        for i in lines:
            row = jnp.broadcast_to(upright[:, i : i + 1], (128, 128)).astype(jnp.int16)
            row = jnp.concatenate([row] * (rows // 128), axis=1)
            hots.append(jnp.where(ids == row, jnp.ones((), BF16), jnp.zeros((), BF16)))
        part = dot(placed(STEPS * near, spot, weighted), jnp.concatenate(hots, axis=0), NN)
        gather_force(force_ref, part, start)

    def add_force(moment):
        state_ref[0, PAD : 3 * PAD] += force_ref[moment * near : (moment + 1) * near]

    backward_steps(state_ref, factor_ref, add_force)
    odd = on_odd_tile()
    for field in range(3):
        west = state_ref[field, PAD - HALO : PAD]
        east = state_ref[field, 3 * PAD : 3 * PAD + HALO]
        put_edge(inner_ref, field, 0, jnp.where(odd, west, east))
        put_edge(outer_ref, field, 0, jnp.where(odd, east, west))


def edge_adjoint(seen, weight, cell, slot, factors, cols):
    rows = factors.shape[1]
    nobs = cell.shape[1]
    return call(
        lambda *refs: edge_adjoint_kernel(*refs, cols=cols),
        "edge_adjoint",
        [floats(1, nobs), floats(2 * STEPS * PAD, rows), edge_floats(rows), edge_floats(rows)],
        [pltpu.VMEM((3, 4 * PAD, rows), F32)],
        10**9,
    )(seen, weight, cell, slot, cell.reshape(nobs // 128, 128), factors)


def adjoint_kernel(
    weighted_ref, edge_ref, cell_ref, slot_ref, factor_ref, adj_ref, state_ref, force_ref
):
    _, cols, rows = adj_ref.shape
    nobs = cell_ref.shape[1]
    count = cols - 2 * PAD
    chunk = 512
    for start in range(0, nobs, chunk):
        here = slice(start, start + chunk)
        row, slot, col = rows_and_spots(cell_ref[:, here], slot_ref[:, here], cols)
        within = (col >= PAD) & (col < cols - PAD)
        spot = jnp.where(within, slot * count + (col - PAD), -1)
        hot = placed(STEPS * count, spot, weighted_ref[:, here])
        gather_force(force_ref, dot(hot, one_hot_rows(row, rows), NT), start)

    def add_force(moment):
        near = 2 * PAD * moment
        state_ref[0, PAD : 2 * PAD] += edge_ref[near : near + PAD]
        state_ref[0, 2 * PAD : cols] += force_ref[moment * count : (moment + 1) * count]
        state_ref[0, cols : PAD + cols] += edge_ref[near + PAD : near + 2 * PAD]

    backward_steps(state_ref, factor_ref, add_force)
    for field in range(3):
        adj_ref[field] = state_ref[field, PAD : PAD + cols]


def tile_adjoint(weighted, edge, cell, slot, factors, cols):
    rows = factors.shape[1]
    return call(
        adjoint_kernel,
        "adjoint",
        floats(3, cols, rows),
        [
            pltpu.VMEM((3, cols + 2 * PAD, rows), F32),
            pltpu.VMEM((STEPS * (cols - 2 * PAD), rows), F32),
        ],
        4 * 10**9,
    )(weighted, edge, cell, slot, factors)


def three_products(parts_ref, high_ref, low_ref, lines):
    both = dot(parts_ref[...], high_ref[...], NN)
    rest = dot(parts_ref[0:lines], low_ref[...], NN)
    return both[0:lines] + both[lines : 2 * lines] + rest


def image_kernel(high_ref, low_ref, adj_ref, pert_ref, dir_ref, img_ref, parts_ref):
    members, cols, rows = dir_ref.shape
    lines = members * cols
    for m in range(members):
        projected = pert_ref[m, 0].astype(F32) * adj_ref[0]
        projected += pert_ref[m, 1].astype(F32) * adj_ref[1]
        projected += pert_ref[m, 2].astype(F32) * adj_ref[2]
        high, low = split_two(projected)
        parts_ref[m * cols : (m + 1) * cols] = high
        parts_ref[lines + m * cols : lines + (m + 1) * cols] = low
    pulled = three_products(parts_ref, high_ref, low_ref, lines)
    img_ref[...] = dir_ref[...] + pulled.reshape(members, cols, rows)


def own_image(high, low, adj, pert, direction):
    members, cols, rows = direction.shape
    return call(
        image_kernel,
        "image",
        floats(members, cols, rows),
        [pltpu.VMEM((2 * members * cols, rows), BF16)],
        10**9,
    )(high, low, adj, pert, direction)


def closing_kernel(
    high_ref, low_ref, own_ref, inner_ref, outer_ref, pert_ref, dir_ref, res_ref, img_ref, sums_ref,
    edge_ref, parts_ref,
):
    members, cols, rows = dir_ref.shape
    near = 2 * PAD
    lines = members * near
    odd = on_odd_tile()
    edge_ref[...] = jnp.zeros(edge_ref.shape, F32)
    for field in range(3):
        inner, outer = get_edge(inner_ref, field), get_edge(outer_ref, field)
        edge_ref[field, 0:HALO] = jnp.where(odd, inner, outer)
        edge_ref[field, near - HALO : near] = jnp.where(odd, outer, inner)
    for m in range(members):
        west = jnp.zeros((PAD, rows), F32)
        east = jnp.zeros((PAD, rows), F32)
        for field in range(3):
            west += pert_ref[m, field, 0:PAD].astype(F32) * edge_ref[field, 0:PAD]
            east += pert_ref[m, field, cols - PAD : cols].astype(F32) * edge_ref[field, PAD:near]
        high, low = split_two(jnp.concatenate([west, east], axis=0))
        parts_ref[m * near : (m + 1) * near] = high
        parts_ref[lines + m * near : lines + (m + 1) * near] = low
    pulled = three_products(parts_ref, high_ref, low_ref, lines)
    totals = [jnp.zeros((8, rows), F32) for _ in range(4)]
    for m in range(members):
        for start in range(0, cols, PAD):
            here = slice(start, start + PAD)
            image = own_ref[m, here]
            if start == 0:
                image = image + pulled[m * near : m * near + PAD]
            if start == cols - PAD:
                image = image + pulled[m * near + PAD : (m + 1) * near]
            img_ref[m, here] = image
            way = dir_ref[m, here]
            left = res_ref[m, here]
            totals[0] += left * left
            totals[1] += way * image
            totals[2] += left * image
            totals[3] += image * image
    lane = lax.broadcasted_iota(jnp.int32, (1, 128), 1)
    packed = jnp.zeros((1, 128), F32)
    for i in range(4):
        total = jnp.sum(jnp.sum(totals[i], axis=0, keepdims=True), axis=1, keepdims=True)
        packed = jnp.where(lane == i, total, packed)
    sums_ref[...] = jnp.broadcast_to(packed, sums_ref.shape)


def image_and_sums(high, low, own, inner, outer, pert, direction, residual, copies):
    members, cols, rows = direction.shape
    return call(
        closing_kernel,
        "closing",
        [floats(members, cols, rows), floats(copies, 128)],
        [
            pltpu.VMEM((3, 2 * PAD, rows), F32),
            pltpu.VMEM((4 * members * PAD, rows), BF16),
        ],
        5 * 10**8,
    )(high, low, own, inner, outer, pert, direction, residual)


def update_kernel(
    sums_ref, control_ref, res_ref, dir_ref, img_ref, control_out, res_out, dir_out, new_ref, sems
):
    members, cols, rows = dir_ref.shape
    total = jnp.sum(sums_ref[...], axis=0, keepdims=True)
    lane = lax.broadcasted_iota(jnp.int32, (1, 128), 1)

    def lane_of(i):
        return jnp.sum(jnp.where(lane == i, total, 0.0), axis=1, keepdims=True)

    norm_old, curvature, cross_term, square = (lane_of(i) for i in range(4))
    step_size = norm_old / curvature
    norm_new = norm_old - 2.0 * step_size * cross_term + step_size * step_size * square
    ratio = norm_new / norm_old
    copies = []
    for m in range(members):
        way = dir_ref[m]
        left = res_ref[m] - step_size * img_ref[m]
        new_ref[0, m] = control_ref[m] + step_size * way
        new_ref[1, m] = left
        new_ref[2, m] = left + ratio * way
        for i, out in enumerate((control_out, res_out, dir_out)):
            copy = pltpu.make_async_copy(new_ref.at[i, m], out.at[m], sems.at[3 * m + i])
            copy.start()
            copies.append(copy)
    for copy in copies:
        copy.wait()


def updated(sums, control, residual, direction, image):
    members = control.shape[0]
    return call(
        update_kernel,
        "update",
        [floats(*control.shape)] * 3,
        [pltpu.VMEM((3, *control.shape), F32), pltpu.SemaphoreType.DMA((3 * members,))],
        10**7,
        out_specs=[HBM, HBM, HBM],
    )(sums, control, residual, direction, image)


def swapped(inner, outer):
    count = lax.axis_size(LON)
    inner_pairs = [(i, i ^ 1) for i in range(count)]
    outer_pairs = [(i, ((i + 1) ^ 1) - 1) for i in range(count)]
    outer_pairs = [(source, target % count) for source, target in outer_pairs]
    return lax.ppermute(inner, LON, inner_pairs), lax.ppermute(outer, LON, outer_pairs)


def body(control, residual, direction, ens_perturb, localize, obs_cell, obs_slot, obs_weight):
    cols = control.shape[2]
    factors = jnp.asarray(grid_factors(localize.shape[0]))
    turned = lambda x: jnp.swapaxes(x, 1, 2)
    control_t, residual_t, direction_t = turned(control), turned(residual), turned(direction)
    pert = jnp.swapaxes(ens_perturb, 2, 3)
    cell, slot, weight = obs_cell[None], obs_slot[None], obs_weight[None]
    inc, inner, outer, high, low = partial_increment(localize, direction_t, pert)
    inner, outer = swapped(inner, outer)
    seen = inner_observed(inc, factors, cell, slot)
    seen = observed_parts(seen, inc, inner, outer, factors, cell, slot, lax.axis_size(ENS))
    seen = lax.all_to_all(seen, ENS, 0, 0, tiled=True)
    weighted, edge, inner, outer = edge_adjoint(seen, weight, cell, slot, factors, cols)
    inner, outer = swapped(inner, outer)
    adj = tile_adjoint(weighted, edge, cell, slot, factors, cols)
    image = own_image(high, low, adj, pert, direction_t)
    image, sums = image_and_sums(
        high, low, image, inner, outer, pert, direction_t, residual_t, lax.axis_size(ENS_LON)
    )
    sums = lax.all_to_all(sums, ENS_LON, 0, 0, tiled=True)
    results = updated(sums, control_t, residual_t, direction_t, image)
    return tuple(turned(x) for x in results)


def solution(mesh):
    split = Mesh(mesh.devices.reshape(2, 4, 8, 2, 2), ("ens_0", "ens_1", "lon_0", "lon_1", "lon_2"))
    placed = (
        P(ENS, None, LON),
        P(ENS, None, LON),
        P(ENS, None, LON),
        P(ENS, None, None, LON),
        P(),
        P(LON),
        P(LON),
        P(LON),
    )
    return jax.shard_map(
        body,
        mesh=split,
        in_specs=placed,
        out_specs=(P(ENS, None, LON), P(ENS, None, LON), P(ENS, None, LON)),
        check_vma=False,
    )
```

```python
import jax
import jax.numpy as jnp
import numpy as np
from jax import lax
from jax.experimental import pallas as pl
from jax.experimental.pallas import tpu as pltpu
from jax.sharding import Mesh
from jax.sharding import PartitionSpec as P

STEPS = 3
HALO = 3
PAD = 8
LON = ("lon_0", "lon_1", "lon_2")
ENS = ("ens_0", "ens_1")
ENS_LON = ("ens_0", "ens_1", "lon_0", "lon_1", "lon_2")

wave_speed = 0.35
rotation = 0.2

F32 = jnp.float32
BF16 = jnp.bfloat16
NT = (((1,), (1,)), ((), ()))
NN = (((1,), (0,)), ((), ()))
HBM = pl.BlockSpec(memory_space=pltpu.HBM)


def split_two(x):
    high = x.astype(BF16)
    low = (x - high.astype(F32)).astype(BF16)
    return high, low


def remainder(x):
    return x - x.astype(BF16).astype(F32)


def dot(a, b, dims):
    return lax.dot_general(a, b, dims, preferred_element_type=F32)


def grid_factors(lat_total):
    row_ids = np.arange(lat_total).astype(np.float32)
    latitude = (-1.0 / 3.0 + 2.0 / 3.0 * (row_ids + 0.5) / lat_total) * np.pi
    return np.stack([1.0 / np.cos(latitude), np.sin(latitude)]).astype(np.float32)


def differences(shape, orient, metric):
    wide, rows = shape
    lane = lax.broadcasted_iota(jnp.int32, (1, rows), 1)
    lon_scale = (orient * wave_speed * 0.5) * metric
    lat_scale = orient * wave_speed * 0.5
    keep_next = jnp.where(lane == rows - 1, 0.0, lat_scale)
    keep_last = jnp.where(lane == 0, 0.0, lat_scale)

    def lon_diff(x):
        return lon_scale * (pltpu.roll(x, wide - 1, 0) - pltpu.roll(x, 1, 0))

    def lat_diff(x):
        return keep_next * pltpu.roll(x, rows - 1, 1) - keep_last * pltpu.roll(x, 1, 1)

    return lon_diff, lat_diff


def model_step(h, u, v, orient, metric, coriolis):
    turn = (orient * rotation) * coriolis
    lon_diff, lat_diff = differences(h.shape, orient, metric)
    return (
        h - (lon_diff(u) + lat_diff(v)),
        u - lon_diff(h) + turn * v,
        v - lat_diff(h) - turn * u,
    )


def first_step(h, orient, metric):
    lon_diff, lat_diff = differences(h.shape, orient, metric)
    return h, -lon_diff(h), -lat_diff(h)


def call(kernel, name, out_shape, scratch, flops, limit_mib=24, **options):
    return pl.pallas_call(
        kernel,
        name=name,
        out_shape=out_shape,
        scratch_shapes=scratch,
        compiler_params=pltpu.CompilerParams(vmem_limit_bytes=limit_mib << 20),
        cost_estimate=pl.CostEstimate(flops=flops, bytes_accessed=1 << 20, transcendentals=0),
        **options,
    )


def floats(*dims):
    return jax.ShapeDtypeStruct(dims, F32)


def rows_and_spots(cell, slot, cols):
    bits = cols.bit_length() - 1
    assert cols == 1 << bits
    return lax.shift_right_logical(cell, bits), slot, cell & (cols - 1)


def one_hot_rows(row, rows):
    ids = lax.broadcasted_iota(jnp.int16, (rows, row.shape[1]), 0)
    return jnp.where(ids == row.astype(jnp.int16), jnp.ones((), BF16), jnp.zeros((), BF16))


def on_odd_tile():
    return lax.axis_index("lon_2") == 1


def put_edge(ref, field, lanes, value):
    for i in range(lanes // 128, lanes // 128 + value.shape[1] // 128):
        line = 3 * HALO * i + HALO * field
        at = i * 128 - lanes
        ref[line : line + HALO] = value[:, at : at + 128]


def get_edge(ref, field):
    tiles = range(ref.shape[0] // (3 * HALO))
    lines = [3 * HALO * i + HALO * field for i in tiles]
    return jnp.concatenate([ref[line : line + HALO] for line in lines], axis=1)


def edge_floats(rows):
    return floats(3 * HALO * rows // 128, 128)


def increment_kernel(
    loc_hbm, dir_hbm, pert_hbm, inc_ref, inner_ref, outer_ref, loc_ref, low_ref,
    dir_ref, pert_ref, parts_ref, sems,
):
    members, cols, rows = dir_ref.shape
    lines = members * cols
    block = 256
    blocks = rows // block
    first = pltpu.make_async_copy(dir_hbm, dir_ref, sems.at[0])
    second = pltpu.make_async_copy(pert_hbm, pert_ref, sems.at[1])
    places = [slice(i * block, (i + 1) * block) for i in range(blocks)]
    copies = [
        pltpu.make_async_copy(loc_hbm.at[here], loc_ref.at[here], sems.at[2 + i])
        for i, here in enumerate(places)
    ]
    odd = on_odd_tile()
    first.start()
    copies[0].start()
    second.start()
    for copy in copies[1:]:
        copy.start()
    first.wait()
    flat = dir_ref[...].reshape(lines, rows)
    parts_ref[0:lines] = flat
    parts_ref[lines : 2 * lines] = remainder(flat)
    for i in range(blocks + 1):
        if i < blocks:
            copies[i].wait()
            low_ref[places[i]] = remainder(loc_ref[places[i]]).astype(BF16)
        if i == 0:
            continue
        if i == 1:
            second.wait()
        here = places[i - 1]
        both = dot(parts_ref[...], loc_ref[here], NT)
        rest = dot(parts_ref[0:lines].astype(BF16), low_ref[here], NT)
        localized = both[0:lines] + both[lines : 2 * lines] + rest
        for field in range(3):
            total = None
            for m in range(members):
                term = pert_ref[m, field, :, here].astype(F32) * localized[m * cols : (m + 1) * cols]
                total = term if total is None else total + term
            inc_ref[field, :, here] = total
            west, east = total[0:HALO], total[cols - HALO : cols]
            put_edge(inner_ref, field, here.start, jnp.where(odd, west, east))
            put_edge(outer_ref, field, here.start, jnp.where(odd, east, west))


def partial_increment(localize, direction, pert):
    members, cols, rows = direction.shape
    low = jax.ShapeDtypeStruct((rows, rows), BF16)
    return call(
        increment_kernel,
        "increment",
        [floats(3, cols, rows), edge_floats(rows), edge_floats(rows), floats(rows, rows), low],
        [
            pltpu.VMEM(direction.shape, F32),
            pltpu.VMEM(pert.shape, BF16),
            pltpu.VMEM((2 * members * cols, rows), F32),
            pltpu.SemaphoreType.DMA((2 + rows // 256,)),
        ],
        10**9,
        in_specs=[HBM, HBM, HBM],
    )(*(pltpu.with_memory_space_constraint(x, pltpu.HBM) for x in (localize, direction, pert)))


def forward_steps(state_ref, factor_ref, parts_ref, places):
    metric = factor_ref[0:1]
    coriolis = factor_ref[1:2]
    count = sum(stop - start for start, stop in places)
    for moment in range(STEPS):
        h, u, v = model_step(state_ref[0], state_ref[1], state_ref[2], 1.0, metric, coriolis)
        if moment + 1 < STEPS:
            state_ref[0] = h
            state_ref[1] = u
            state_ref[2] = v
        line = moment * count
        for start, stop in places:
            high, low = split_two(h[start:stop])
            parts_ref[line : line + stop - start] = high
            parts_ref[STEPS * count + line : STEPS * count + line + stop - start] = low
            line += stop - start


def sampled(parts_ref, row, spot, rows):
    spots = parts_ref.shape[0] // 2
    picked = dot(parts_ref[...], one_hot_rows(row, rows), NN)
    picked = picked[0:spots] + picked[spots : 2 * spots]
    spot_hot = lax.broadcasted_iota(jnp.int32, picked.shape, 0) == spot
    return jnp.sum(jnp.where(spot_hot, picked, 0.0), axis=0, keepdims=True)


def forward_kernel(inc_ref, factor_ref, cell_ref, slot_ref, out_ref, state_ref, parts_ref):
    _, cols, rows = inc_ref.shape
    nobs = cell_ref.shape[1]
    state_ref[...] = inc_ref[...]
    forward_steps(state_ref, factor_ref, parts_ref, ((PAD, cols - PAD),))
    chunk = 512
    for start in range(0, nobs, chunk):
        here = slice(start, start + chunk)
        row, slot, col = rows_and_spots(cell_ref[:, here], slot_ref[:, here], cols)
        within = (col >= PAD) & (col < cols - PAD)
        spot = jnp.where(within, slot * (cols - 2 * PAD) + (col - PAD), -1)
        out_ref[:, here] = sampled(parts_ref, row, spot, rows)


def inner_observed(inc, factors, cell, slot):
    _, cols, rows = inc.shape
    return call(
        forward_kernel,
        "forward",
        floats(1, cell.shape[1]),
        [
            pltpu.VMEM((3, cols, rows), F32),
            pltpu.VMEM((2 * STEPS * (cols - 2 * PAD), rows), BF16),
        ],
        4 * 10**9,
    )(inc, factors, cell, slot)


def border_kernel(
    seen_ref, inc_ref, inner_ref, outer_ref, factor_ref, cell_ref, slot_ref, out_ref,
    state_ref, parts_ref,
):
    _, cols, rows = inc_ref.shape
    nobs = cell_ref.shape[1]
    odd = on_odd_tile()
    state_ref[...] = jnp.zeros(state_ref.shape, F32)
    for field in range(3):
        inner, outer = get_edge(inner_ref, field), get_edge(outer_ref, field)
        state_ref[field, PAD - HALO : PAD] = jnp.where(odd, inner, outer)
        state_ref[field, PAD : 3 * PAD] = inc_ref[field, 0 : 2 * PAD]
        state_ref[field, 3 * PAD : 5 * PAD] = inc_ref[field, cols - 2 * PAD : cols]
        state_ref[field, 5 * PAD : 5 * PAD + HALO] = jnp.where(odd, outer, inner)
    forward_steps(state_ref, factor_ref, parts_ref, ((PAD, 2 * PAD), (4 * PAD, 5 * PAD)))
    near = 2 * PAD
    chunk = 512
    for start in range(0, nobs, chunk):
        here = slice(start, start + chunk)
        row, slot, col = rows_and_spots(cell_ref[:, here], slot_ref[:, here], cols)
        east_spot = jnp.where(col >= cols - PAD, slot * near + (col - cols + near), -1)
        spot = jnp.where(col < PAD, slot * near + col, east_spot)
        value = sampled(parts_ref, row, spot, rows) + seen_ref[:, here]
        for i in range(0, chunk, 128):
            line = (start + i) // 128
            out_ref[:, line, :] = jnp.broadcast_to(value[:, i : i + 128], (out_ref.shape[0], 128))


def observed_parts(seen, inc, inner, outer, factors, cell, slot, copies):
    rows = inc.shape[2]
    return call(
        border_kernel,
        "border",
        floats(copies, cell.shape[1] // 128, 128),
        [
            pltpu.VMEM((3, 6 * PAD, rows), F32),
            pltpu.VMEM((4 * STEPS * PAD, rows), BF16),
        ],
        10**9,
    )(seen, inc, inner, outer, factors, cell, slot)


def backward_steps(state_ref, factor_ref, add_force):
    metric = factor_ref[0:1]
    coriolis = factor_ref[1:2]
    state_ref[0] = jnp.zeros(state_ref.shape[1:], F32)
    for moment in reversed(range(STEPS)):
        add_force(moment)
        if moment == STEPS - 1:
            h, u, v = first_step(state_ref[0], -1.0, metric)
        else:
            h, u, v = model_step(state_ref[0], state_ref[1], state_ref[2], -1.0, metric, coriolis)
        state_ref[0] = h
        state_ref[1] = u
        state_ref[2] = v


def placed(spots, spot, weighted):
    spot_hot = lax.broadcasted_iota(jnp.int32, (spots, spot.shape[1]), 0) == spot
    return jnp.concatenate(split_two(jnp.where(spot_hot, weighted, 0.0)), axis=0)


def gather_force(force_ref, part, start):
    spots = force_ref.shape[0]
    part = part[0:spots] + part[spots : 2 * spots]
    if start == 0:
        force_ref[...] = part
    else:
        force_ref[...] += part


def edge_adjoint_kernel(
    seen_ref, weight_ref, cell_ref, slot_ref, lines_ref, factor_ref,
    weighted_ref, force_ref, inner_ref, outer_ref, state_ref, *, cols,
):
    rows = factor_ref.shape[1]
    nobs = cell_ref.shape[1]
    near = 2 * PAD
    chunk = 512
    seen = jnp.sum(seen_ref[...], axis=0)
    upright = jnp.transpose(lax.shift_right_logical(lines_ref[...], cols.bit_length() - 1))
    ids = lax.broadcasted_iota(jnp.int16, (128, rows), 1)
    for start in range(0, nobs, chunk):
        here = slice(start, start + chunk)
        _, slot, col = rows_and_spots(cell_ref[:, here], slot_ref[:, here], cols)
        lines = range(start // 128, (start + chunk) // 128)
        weighted = weight_ref[:, here] * jnp.concatenate([seen[i : i + 1] for i in lines], axis=1)
        weighted_ref[:, here] = weighted
        east_spot = jnp.where(col >= cols - PAD, slot * near + (col - cols + near), -1)
        spot = jnp.where(col < PAD, slot * near + col, east_spot)
        hots = []
        for i in lines:
            row = jnp.broadcast_to(upright[:, i : i + 1], (128, 128)).astype(jnp.int16)
            row = jnp.concatenate([row] * (rows // 128), axis=1)
            hots.append(jnp.where(ids == row, jnp.ones((), BF16), jnp.zeros((), BF16)))
        part = dot(placed(STEPS * near, spot, weighted), jnp.concatenate(hots, axis=0), NN)
        gather_force(force_ref, part, start)

    def add_force(moment):
        state_ref[0, PAD : 3 * PAD] += force_ref[moment * near : (moment + 1) * near]

    backward_steps(state_ref, factor_ref, add_force)
    odd = on_odd_tile()
    for field in range(3):
        west = state_ref[field, PAD - HALO : PAD]
        east = state_ref[field, 3 * PAD : 3 * PAD + HALO]
        put_edge(inner_ref, field, 0, jnp.where(odd, west, east))
        put_edge(outer_ref, field, 0, jnp.where(odd, east, west))


def edge_adjoint(seen, weight, cell, slot, factors, cols):
    rows = factors.shape[1]
    nobs = cell.shape[1]
    return call(
        lambda *refs: edge_adjoint_kernel(*refs, cols=cols),
        "edge_adjoint",
        [floats(1, nobs), floats(2 * STEPS * PAD, rows), edge_floats(rows), edge_floats(rows)],
        [pltpu.VMEM((3, 4 * PAD, rows), F32)],
        10**9,
    )(seen, weight, cell, slot, cell.reshape(nobs // 128, 128), factors)


def three_products(parts_ref, loc_ref, low_ref, lines):
    both = dot(parts_ref[...], loc_ref[...], NN)
    rest = dot(parts_ref[0:lines].astype(BF16), low_ref[...], NN)
    return both[0:lines] + both[lines : 2 * lines] + rest


def adjoint_kernel(
    weighted_ref, edge_ref, cell_ref, slot_ref, factor_ref, loc_ref, low_ref, pert_ref, dir_ref,
    img_ref, state_ref, force_ref, parts_ref,
):
    members, cols, rows = dir_ref.shape
    nobs = cell_ref.shape[1]
    count = cols - 2 * PAD
    chunk = 512
    for start in range(0, nobs, chunk):
        here = slice(start, start + chunk)
        row, slot, col = rows_and_spots(cell_ref[:, here], slot_ref[:, here], cols)
        within = (col >= PAD) & (col < cols - PAD)
        spot = jnp.where(within, slot * count + (col - PAD), -1)
        hot = placed(STEPS * count, spot, weighted_ref[:, here])
        gather_force(force_ref, dot(hot, one_hot_rows(row, rows), NT), start)

    def add_force(moment):
        near = 2 * PAD * moment
        state_ref[0, PAD : 2 * PAD] += edge_ref[near : near + PAD]
        state_ref[0, 2 * PAD : cols] += force_ref[moment * count : (moment + 1) * count]
        state_ref[0, cols : PAD + cols] += edge_ref[near + PAD : near + 2 * PAD]

    backward_steps(state_ref, factor_ref, add_force)
    lines = members * cols
    for m in range(members):
        projected = pert_ref[m, 0].astype(F32) * state_ref[0, PAD : PAD + cols]
        projected += pert_ref[m, 1].astype(F32) * state_ref[1, PAD : PAD + cols]
        projected += pert_ref[m, 2].astype(F32) * state_ref[2, PAD : PAD + cols]
        parts_ref[m * cols : (m + 1) * cols] = projected
        parts_ref[lines + m * cols : lines + (m + 1) * cols] = remainder(projected)
    pulled = three_products(parts_ref, loc_ref, low_ref, lines)
    img_ref[...] = dir_ref[...] + pulled.reshape(members, cols, rows)


def own_image(weighted, edge, cell, slot, factors, loc, low, pert, direction):
    members, cols, rows = direction.shape
    return call(
        adjoint_kernel,
        "adjoint",
        floats(members, cols, rows),
        [
            pltpu.VMEM((3, cols + 2 * PAD, rows), F32),
            pltpu.VMEM((STEPS * (cols - 2 * PAD), rows), F32),
            pltpu.VMEM((2 * members * cols, rows), F32),
        ],
        4 * 10**9,
    )(weighted, edge, cell, slot, factors, loc, low, pert, direction)


def closing_kernel(
    loc_ref, low_ref, own_ref, inner_ref, outer_ref, pert_ref, dir_ref, res_ref, img_ref, sums_ref,
    edge_ref, parts_ref,
):
    members, cols, rows = dir_ref.shape
    near = 2 * PAD
    lines = members * near
    odd = on_odd_tile()
    edge_ref[...] = jnp.zeros(edge_ref.shape, F32)
    for field in range(3):
        inner, outer = get_edge(inner_ref, field), get_edge(outer_ref, field)
        edge_ref[field, 0:HALO] = jnp.where(odd, inner, outer)
        edge_ref[field, near - HALO : near] = jnp.where(odd, outer, inner)
    for m in range(members):
        west = jnp.zeros((PAD, rows), F32)
        east = jnp.zeros((PAD, rows), F32)
        for field in range(3):
            west += pert_ref[m, field, 0:PAD].astype(F32) * edge_ref[field, 0:PAD]
            east += pert_ref[m, field, cols - PAD : cols].astype(F32) * edge_ref[field, PAD:near]
        projected = jnp.concatenate([west, east], axis=0)
        parts_ref[m * near : (m + 1) * near] = projected
        parts_ref[lines + m * near : lines + (m + 1) * near] = remainder(projected)
    pulled = three_products(parts_ref, loc_ref, low_ref, lines)
    totals = [jnp.zeros((8, rows), F32) for _ in range(4)]
    for m in range(members):
        for start in range(0, cols, PAD):
            here = slice(start, start + PAD)
            image = own_ref[m, here]
            if start == 0:
                image = image + pulled[m * near : m * near + PAD]
            if start == cols - PAD:
                image = image + pulled[m * near + PAD : (m + 1) * near]
            img_ref[m, here] = image
            way = dir_ref[m, here]
            left = res_ref[m, here]
            totals[0] += left * left
            totals[1] += way * image
            totals[2] += left * image
            totals[3] += image * image
    lane = lax.broadcasted_iota(jnp.int32, (1, 128), 1)
    packed = jnp.zeros((1, 128), F32)
    for i in range(4):
        total = jnp.sum(jnp.sum(totals[i], axis=0, keepdims=True), axis=1, keepdims=True)
        packed = jnp.where(lane == i, total, packed)
    sums_ref[...] = jnp.broadcast_to(packed, sums_ref.shape)


def image_and_sums(loc, low, own, inner, outer, pert, direction, residual, copies):
    members, cols, rows = direction.shape
    return call(
        closing_kernel,
        "closing",
        [floats(members, cols, rows), floats(copies, 128)],
        [
            pltpu.VMEM((3, 2 * PAD, rows), F32),
            pltpu.VMEM((4 * members * PAD, rows), F32),
        ],
        5 * 10**8,
    )(loc, low, own, inner, outer, pert, direction, residual)


def update_kernel(
    sums_ref, control_ref, res_ref, dir_ref, img_ref, control_out, res_out, dir_out, new_ref, sems
):
    members, cols, rows = dir_ref.shape
    total = jnp.sum(sums_ref[...], axis=0, keepdims=True)
    lane = lax.broadcasted_iota(jnp.int32, (1, 128), 1)

    def lane_of(i):
        return jnp.sum(jnp.where(lane == i, total, 0.0), axis=1, keepdims=True)

    norm_old, curvature, cross_term, square = (lane_of(i) for i in range(4))
    step_size = norm_old / curvature
    norm_new = norm_old - 2.0 * step_size * cross_term + step_size * step_size * square
    ratio = norm_new / norm_old
    copies = []
    for m in range(members):
        way = dir_ref[m]
        left = res_ref[m] - step_size * img_ref[m]
        new_ref[0, m] = control_ref[m] + step_size * way
        new_ref[1, m] = left
        new_ref[2, m] = left + ratio * way
        for i, out in enumerate((control_out, res_out, dir_out)):
            copy = pltpu.make_async_copy(new_ref.at[i, m], out.at[m], sems.at[3 * m + i])
            copy.start()
            copies.append(copy)
    for copy in copies:
        copy.wait()


def updated(sums, control, residual, direction, image):
    members = control.shape[0]
    return call(
        update_kernel,
        "update",
        [floats(*control.shape)] * 3,
        [pltpu.VMEM((3, *control.shape), F32), pltpu.SemaphoreType.DMA((3 * members,))],
        10**7,
        out_specs=[HBM, HBM, HBM],
    )(sums, control, residual, direction, image)


def swapped(inner, outer):
    count = lax.axis_size(LON)
    inner_pairs = [(i, i ^ 1) for i in range(count)]
    outer_pairs = [(i, ((i + 1) ^ 1) - 1) for i in range(count)]
    outer_pairs = [(source, target % count) for source, target in outer_pairs]
    return lax.ppermute(inner, LON, inner_pairs), lax.ppermute(outer, LON, outer_pairs)


def body(control, residual, direction, ens_perturb, localize, obs_cell, obs_slot, obs_weight):
    cols = control.shape[2]
    factors = jnp.asarray(grid_factors(localize.shape[0]))
    turned = lambda x: jnp.swapaxes(x, 1, 2)
    control_t, residual_t, direction_t = turned(control), turned(residual), turned(direction)
    pert = jnp.swapaxes(ens_perturb, 2, 3)
    cell, slot, weight = obs_cell[None], obs_slot[None], obs_weight[None]
    inc, inner, outer, loc, low = partial_increment(localize, direction_t, pert)
    inner, outer = swapped(inner, outer)
    seen = inner_observed(inc, factors, cell, slot)
    seen = observed_parts(seen, inc, inner, outer, factors, cell, slot, lax.axis_size(ENS))
    seen = lax.all_to_all(seen, ENS, 0, 0, tiled=True)
    weighted, edge, inner, outer = edge_adjoint(seen, weight, cell, slot, factors, cols)
    inner, outer = swapped(inner, outer)
    image = own_image(
        weighted, edge, cell, slot, factors, loc, low, pert, direction_t
    )
    image, sums = image_and_sums(
        loc, low, image, inner, outer, pert, direction_t, residual_t, lax.axis_size(ENS_LON)
    )
    sums = lax.all_to_all(sums, ENS_LON, 0, 0, tiled=True)
    results = updated(sums, control_t, residual_t, direction_t, image)
    return tuple(turned(x) for x in results)


def solution(mesh):
    split = Mesh(mesh.devices.reshape(2, 4, 8, 2, 2), ("ens_0", "ens_1", "lon_0", "lon_1", "lon_2"))
    placed = (
        P(ENS, None, LON),
        P(ENS, None, LON),
        P(ENS, None, LON),
        P(ENS, None, None, LON),
        P(),
        P(LON),
        P(LON),
        P(LON),
    )
    return jax.shard_map(
        body,
        mesh=split,
        in_specs=placed,
        out_specs=(P(ENS, None, LON), P(ENS, None, LON), P(ENS, None, LON)),
        check_vma=False,
    )
```

```python
import jax
import jax.numpy as jnp
import numpy as np
from jax import lax
from jax.experimental import pallas as pl
from jax.experimental.pallas import tpu as pltpu
from jax.sharding import Mesh
from jax.sharding import PartitionSpec as P

STEPS = 3
HALO = 3
REACH = 2 * HALO
CORNER = HALO * (HALO + 1) // 2
PAD = 8
LON = ("lon_0", "lon_1", "lon_2")
ENS = ("ens_0", "ens_1")
ENS_LON = ("ens_0", "ens_1", "lon_0", "lon_1", "lon_2")

wave_speed = 0.35
rotation = 0.2

F32 = jnp.float32
BF16 = jnp.bfloat16
NT = (((1,), (1,)), ((), ()))
NN = (((1,), (0,)), ((), ()))
HBM = pl.BlockSpec(memory_space=pltpu.HBM)


def split_two(x):
    high = x.astype(BF16)
    low = (x - high.astype(F32)).astype(BF16)
    return high, low


def remainder(x):
    return x - x.astype(BF16).astype(F32)


def dot(a, b, dims):
    return lax.dot_general(a, b, dims, preferred_element_type=F32)


def grid_factors(lat_total):
    row_ids = np.arange(lat_total).astype(np.float32)
    latitude = (-1.0 / 3.0 + 2.0 / 3.0 * (row_ids + 0.5) / lat_total) * np.pi
    return np.stack([1.0 / np.cos(latitude), np.sin(latitude)]).astype(np.float32)


def differences(shape, orient, metric):
    wide, rows = shape
    lane = lax.broadcasted_iota(jnp.int32, (1, rows), 1)
    lon_scale = (orient * wave_speed * 0.5) * metric
    lat_scale = orient * wave_speed * 0.5
    keep_next = jnp.where(lane == rows - 1, 0.0, lat_scale)
    keep_last = jnp.where(lane == 0, 0.0, lat_scale)

    def lon_diff(x):
        return lon_scale * (pltpu.roll(x, wide - 1, 0) - pltpu.roll(x, 1, 0))

    def lat_diff(x):
        return keep_next * pltpu.roll(x, rows - 1, 1) - keep_last * pltpu.roll(x, 1, 1)

    return lon_diff, lat_diff


def model_step(h, u, v, orient, metric, coriolis):
    turn = (orient * rotation) * coriolis
    lon_diff, lat_diff = differences(h.shape, orient, metric)
    return (
        h - (lon_diff(u) + lat_diff(v)),
        u - lon_diff(h) + turn * v,
        v - lat_diff(h) - turn * u,
    )


def first_step(h, orient, metric):
    lon_diff, lat_diff = differences(h.shape, orient, metric)
    return h, -lon_diff(h), -lat_diff(h)


def call(kernel, name, out_shape, scratch, flops, limit_mib=24, **options):
    return pl.pallas_call(
        kernel,
        name=name,
        out_shape=out_shape,
        scratch_shapes=scratch,
        compiler_params=pltpu.CompilerParams(vmem_limit_bytes=limit_mib << 20),
        cost_estimate=pl.CostEstimate(flops=flops, bytes_accessed=1 << 20, transcendentals=0),
        **options,
    )


def floats(*dims):
    return jax.ShapeDtypeStruct(dims, F32)


def rows_and_spots(cell, slot, cols):
    bits = cols.bit_length() - 1
    assert cols == 1 << bits
    return lax.shift_right_logical(cell, bits), slot, cell & (cols - 1)


def one_hot_rows(row, rows):
    ids = lax.broadcasted_iota(jnp.int16, (rows, row.shape[1]), 0)
    return jnp.where(ids == row.astype(jnp.int16), jnp.ones((), BF16), jnp.zeros((), BF16))


def on_odd_tile():
    return lax.axis_index("lon_2") == 1


def corner(moment):
    first = moment * (moment + 1) // 2
    return slice(first, first + moment + 1)


def edge_floats(rows):
    return floats(3 * REACH + CORNER, rows)


def from_sides(inner, outer):
    odd = on_odd_tile()
    return jnp.where(odd, inner, outer), jnp.where(odd, outer, inner)


def placed(spots, spot, weighted):
    spot_hot = lax.broadcasted_iota(jnp.int32, (spots, spot.shape[1]), 0) == spot
    return jnp.concatenate(split_two(jnp.where(spot_hot, weighted, 0.0)), axis=0)


def gather_force(force_ref, part, start):
    spots = force_ref.shape[0]
    part = part[0:spots] + part[spots : 2 * spots]
    if start == 0:
        force_ref[...] = part
    else:
        force_ref[...] += part


def edge_weights(sum_ref, cell, slot, weight, cols):
    rows = sum_ref.shape[1]
    upright = jnp.transpose(lax.shift_right_logical(cell, cols.bit_length() - 1))
    ids = lax.broadcasted_iota(jnp.int16, (128, rows), 1)
    for start in range(0, cell.shape[0], 4):
        lines = range(start, start + 4)
        cell_at, slot_at, weight_at = (
            jnp.concatenate([x[i : i + 1] for i in lines], axis=1) for x in (cell, slot, weight)
        )
        _, _, col = rows_and_spots(cell_at, slot_at, cols)
        first = lax.shift_right_logical(slot_at * (slot_at + 1), 1)
        from_east = col - (cols - 1 - slot_at)
        spot = jnp.where(from_east >= 0, CORNER + first + from_east, -1)
        spot = jnp.where(col <= slot_at, first + col, spot)
        spot = jnp.where(slot_at < STEPS, spot, -1)
        hots = []
        for i in lines:
            row = jnp.broadcast_to(upright[:, i : i + 1], (128, 128)).astype(jnp.int16)
            row = jnp.concatenate([row] * (rows // 128), axis=1)
            hots.append(jnp.where(ids == row, jnp.ones((), BF16), jnp.zeros((), BF16)))
        part = dot(placed(sum_ref.shape[0], spot, weight_at), jnp.concatenate(hots, axis=0), NN)
        gather_force(sum_ref, part, start)


def increment_kernel(
    loc_hbm, dir_hbm, pert_hbm, cell_hbm, slot_hbm, weight_hbm,
    inc_ref, inner_ref, outer_ref, loc_ref, low_ref,
    dir_ref, pert_ref, parts_ref, cell_ref, slot_ref, weight_ref, sum_ref, sems,
):
    members, cols, rows = dir_ref.shape
    lines = members * cols
    block = 256
    blocks = rows // block
    first = pltpu.make_async_copy(dir_hbm, dir_ref, sems.at[0])
    second = pltpu.make_async_copy(pert_hbm, pert_ref, sems.at[1])
    places = [slice(i * block, (i + 1) * block) for i in range(blocks)]
    copies = [
        pltpu.make_async_copy(loc_hbm.at[here], loc_ref.at[here], sems.at[2 + i])
        for i, here in enumerate(places)
    ]
    lists = [
        pltpu.make_async_copy(source, target, sems.at[2 + blocks + i])
        for i, (source, target) in enumerate(
            ((cell_hbm, cell_ref), (slot_hbm, slot_ref), (weight_hbm, weight_ref))
        )
    ]
    odd = on_odd_tile()
    for copy in lists:
        copy.start()
    first.start()
    copies[0].start()
    second.start()
    for copy in copies[1:]:
        copy.start()
    for copy in lists:
        copy.wait()
    edge_weights(sum_ref, cell_ref[...], slot_ref[...], weight_ref[...], cols)
    west, east = sum_ref[0:CORNER], sum_ref[CORNER : 2 * CORNER]
    inner_ref[3 * REACH : 3 * REACH + CORNER] = jnp.where(odd, west, east)
    outer_ref[3 * REACH : 3 * REACH + CORNER] = jnp.where(odd, east, west)
    first.wait()
    flat = dir_ref[...].reshape(lines, rows)
    parts_ref[0:lines] = flat
    parts_ref[lines : 2 * lines] = remainder(flat)
    for i in range(blocks + 1):
        if i < blocks:
            copies[i].wait()
            low_ref[places[i]] = remainder(loc_ref[places[i]]).astype(BF16)
        if i == 0:
            continue
        if i == 1:
            second.wait()
        here = places[i - 1]
        both = dot(parts_ref[...], loc_ref[here], NT)
        rest = dot(parts_ref[0:lines].astype(BF16), low_ref[here], NT)
        localized = both[0:lines] + both[lines : 2 * lines] + rest
        for field in range(3):
            total = None
            for m in range(members):
                term = pert_ref[m, field, :, here].astype(F32) * localized[m * cols : (m + 1) * cols]
                total = term if total is None else total + term
            inc_ref[field, :, here] = total
            west, east = total[0:REACH], total[cols - REACH : cols]
            inner_ref[REACH * field : REACH * (field + 1), here] = jnp.where(odd, west, east)
            outer_ref[REACH * field : REACH * (field + 1), here] = jnp.where(odd, east, west)


def partial_increment(localize, direction, pert, lists):
    members, cols, rows = direction.shape
    low = jax.ShapeDtypeStruct((rows, rows), BF16)
    return call(
        increment_kernel,
        "increment",
        [floats(3, cols, rows), edge_floats(rows), edge_floats(rows), floats(rows, rows), low],
        [
            pltpu.VMEM(direction.shape, F32),
            pltpu.VMEM(pert.shape, BF16),
            pltpu.VMEM((2 * members * cols, rows), F32),
            *(pltpu.VMEM(x.shape, x.dtype) for x in lists),
            pltpu.VMEM((16, rows), F32),
            pltpu.SemaphoreType.DMA((2 + rows // 256 + len(lists),)),
        ],
        10**9,
        in_specs=[HBM] * (3 + len(lists)),
    )(
        *(
            pltpu.with_memory_space_constraint(x, pltpu.HBM)
            for x in (localize, direction, pert, *lists)
        )
    )


def forward_steps(state_ref, factor_ref, parts_ref, places, keep=None):
    metric = factor_ref[0:1]
    coriolis = factor_ref[1:2]
    count = sum(stop - start for start, stop in places)
    for moment in range(STEPS):
        h, u, v = model_step(state_ref[0], state_ref[1], state_ref[2], 1.0, metric, coriolis)
        if moment + 1 < STEPS:
            state_ref[0] = h
            state_ref[1] = u
            state_ref[2] = v
        if keep is not None:
            keep(moment, h)
        line = moment * count
        for start, stop in places:
            high, low = split_two(h[start:stop])
            parts_ref[line : line + stop - start] = high
            parts_ref[STEPS * count + line : STEPS * count + line + stop - start] = low
            line += stop - start


def sampled(parts_ref, row, spot, rows):
    spots = parts_ref.shape[0] // 2
    picked = dot(parts_ref[...], one_hot_rows(row, rows), NN)
    picked = picked[0:spots] + picked[spots : 2 * spots]
    spot_hot = lax.broadcasted_iota(jnp.int32, picked.shape, 0) == spot
    return jnp.sum(jnp.where(spot_hot, picked, 0.0), axis=0, keepdims=True)


def forward_kernel(inc_ref, factor_ref, cell_ref, slot_ref, out_ref, state_ref, parts_ref):
    _, cols, rows = inc_ref.shape
    nobs = cell_ref.shape[1]
    state_ref[...] = inc_ref[...]
    forward_steps(state_ref, factor_ref, parts_ref, ((PAD, cols - PAD),))
    chunk = 512
    for start in range(0, nobs, chunk):
        here = slice(start, start + chunk)
        row, slot, col = rows_and_spots(cell_ref[:, here], slot_ref[:, here], cols)
        within = (col >= PAD) & (col < cols - PAD)
        spot = jnp.where(within, slot * (cols - 2 * PAD) + (col - PAD), -1)
        out_ref[:, here] = sampled(parts_ref, row, spot, rows)


def inner_observed(inc, factors, cell, slot):
    _, cols, rows = inc.shape
    return call(
        forward_kernel,
        "forward",
        floats(1, cell.shape[1]),
        [
            pltpu.VMEM((3, cols, rows), F32),
            pltpu.VMEM((2 * STEPS * (cols - 2 * PAD), rows), BF16),
        ],
        4 * 10**9,
    )(inc, factors, cell, slot)


def border_kernel(
    seen_ref, inc_ref, inner_ref, outer_ref, factor_ref, cell_ref, slot_ref, out_ref,
    state_ref, parts_ref, halo_ref,
):
    _, cols, rows = inc_ref.shape
    nobs = cell_ref.shape[1]
    state_ref[...] = jnp.zeros(state_ref.shape, F32)
    for field in range(3):
        edge = slice(REACH * field, REACH * (field + 1))
        west, east = from_sides(inner_ref[edge], outer_ref[edge])
        state_ref[field, PAD - REACH : PAD] = west
        state_ref[field, PAD : 3 * PAD] = inc_ref[field, 0 : 2 * PAD]
        state_ref[field, 3 * PAD : 5 * PAD] = inc_ref[field, cols - 2 * PAD : cols]
        state_ref[field, 5 * PAD : 5 * PAD + REACH] = east

    def keep(moment, h):
        at = corner(moment)
        halo_ref[at] = h[PAD - moment - 1 : PAD]
        halo_ref[CORNER + at.start : CORNER + at.stop] = h[5 * PAD : 5 * PAD + moment + 1]

    places = ((PAD, 2 * PAD), (4 * PAD, 5 * PAD))
    forward_steps(state_ref, factor_ref, parts_ref, places, keep)
    copies = out_ref.shape[0]
    tiles = rows // 128
    base = nobs // 128
    for i in range(tiles):
        lanes = slice(128 * i, 128 * (i + 1))
        for first, height in ((0, 8), (8, 4)):
            line = base + first * tiles + height * i
            value = halo_ref[first : first + height, lanes]
            out_ref[:, line : line + height, :] = jnp.broadcast_to(value[None], (copies, height, 128))
    near = 2 * PAD
    chunk = 512
    for start in range(0, nobs, chunk):
        here = slice(start, start + chunk)
        row, slot, col = rows_and_spots(cell_ref[:, here], slot_ref[:, here], cols)
        east_spot = jnp.where(col >= cols - PAD, slot * near + (col - cols + near), -1)
        spot = jnp.where(col < PAD, slot * near + col, east_spot)
        value = sampled(parts_ref, row, spot, rows) + seen_ref[:, here]
        for i in range(0, chunk, 128):
            line = (start + i) // 128
            out_ref[:, line, :] = jnp.broadcast_to(value[:, i : i + 128], (out_ref.shape[0], 128))


def observed_parts(seen, inc, inner, outer, factors, cell, slot, copies):
    rows = inc.shape[2]
    return call(
        border_kernel,
        "border",
        floats(copies, (cell.shape[1] + 2 * CORNER * rows) // 128, 128),
        [
            pltpu.VMEM((3, 6 * PAD, rows), F32),
            pltpu.VMEM((4 * STEPS * PAD, rows), BF16),
            pltpu.VMEM((16, rows), F32),
        ],
        10**9,
    )(seen, inc, inner, outer, factors, cell, slot)


def backward_steps(state_ref, factor_ref, add_force):
    metric = factor_ref[0:1]
    coriolis = factor_ref[1:2]
    state_ref[0] = jnp.zeros(state_ref.shape[1:], F32)
    for moment in reversed(range(STEPS)):
        add_force(moment)
        if moment == STEPS - 1:
            h, u, v = first_step(state_ref[0], -1.0, metric)
        else:
            h, u, v = model_step(state_ref[0], state_ref[1], state_ref[2], -1.0, metric, coriolis)
        state_ref[0] = h
        state_ref[1] = u
        state_ref[2] = v


def three_products(parts_ref, loc_ref, low_ref, lines):
    both = dot(parts_ref[...], loc_ref[...], NN)
    rest = dot(parts_ref[0:lines].astype(BF16), low_ref[...], NN)
    return both[0:lines] + both[lines : 2 * lines] + rest


def finish_kernel(
    seen_ref, weight_ref, cell_ref, slot_ref, inner_ref, outer_ref, factor_ref, loc_ref, low_ref,
    pert_ref, dir_ref, res_ref, img_ref, sums_ref, state_ref, force_ref, parts_ref, halo_ref,
):
    members, cols, rows = dir_ref.shape
    nobs = cell_ref.shape[1]
    spots = STEPS * cols
    chunk = 512
    tiles = rows // 128
    base = nobs // 128
    seen = jnp.sum(seen_ref[...], axis=0)
    for first, height in ((0, 8), (8, 4)):
        lines = [base + first * tiles + height * i for i in range(tiles)]
        halo_ref[first : first + height] = jnp.concatenate(
            [seen[i : i + height] for i in lines], axis=1
        )
    tail = slice(3 * REACH, 3 * REACH + CORNER)
    west, east = from_sides(inner_ref[tail], outer_ref[tail])
    halo_ref[0:CORNER] *= west
    halo_ref[CORNER : 2 * CORNER] *= east
    for start in range(0, nobs, chunk):
        here = slice(start, start + chunk)
        row, slot, col = rows_and_spots(cell_ref[:, here], slot_ref[:, here], cols)
        lines = range(start // 128, (start + chunk) // 128)
        weighted = weight_ref[:, here] * jnp.concatenate([seen[i : i + 1] for i in lines], axis=1)
        hot = placed(spots, slot * cols + col, weighted)
        gather_force(force_ref, dot(hot, one_hot_rows(row, rows), NT), start)

    def add_force(moment):
        at = corner(moment)
        state_ref[0, PAD - moment - 1 : PAD] += halo_ref[at]
        state_ref[0, PAD : PAD + cols] += force_ref[moment * cols : (moment + 1) * cols]
        state_ref[0, PAD + cols : PAD + cols + moment + 1] += halo_ref[
            CORNER + at.start : CORNER + at.stop
        ]

    backward_steps(state_ref, factor_ref, add_force)
    lines = members * cols
    for m in range(members):
        projected = pert_ref[m, 0].astype(F32) * state_ref[0, PAD : PAD + cols]
        projected += pert_ref[m, 1].astype(F32) * state_ref[1, PAD : PAD + cols]
        projected += pert_ref[m, 2].astype(F32) * state_ref[2, PAD : PAD + cols]
        parts_ref[m * cols : (m + 1) * cols] = projected
        parts_ref[lines + m * cols : lines + (m + 1) * cols] = remainder(projected)
    pulled = three_products(parts_ref, loc_ref, low_ref, lines)
    img_ref[...] = dir_ref[...] + pulled.reshape(members, cols, rows)
    totals = [jnp.zeros((8, rows), F32) for _ in range(4)]
    for m in range(members):
        for start in range(0, cols, 8):
            here = slice(start, start + 8)
            image, way, left = img_ref[m, here], dir_ref[m, here], res_ref[m, here]
            totals[0] += left * left
            totals[1] += way * image
            totals[2] += left * image
            totals[3] += image * image
    lane = lax.broadcasted_iota(jnp.int32, (1, 128), 1)
    packed = jnp.zeros((1, 128), F32)
    for i in range(4):
        total = jnp.sum(jnp.sum(totals[i], axis=0, keepdims=True), axis=1, keepdims=True)
        packed = jnp.where(lane == i, total, packed)
    sums_ref[...] = jnp.broadcast_to(packed, sums_ref.shape)


def image_and_sums(
    seen, weight, cell, slot, inner, outer, factors, loc, low, pert, direction, residual, copies
):
    members, cols, rows = direction.shape
    return call(
        finish_kernel,
        "finish",
        [floats(members, cols, rows), floats(copies, 128)],
        [
            pltpu.VMEM((3, cols + 2 * PAD, rows), F32),
            pltpu.VMEM((STEPS * cols, rows), F32),
            pltpu.VMEM((2 * members * cols, rows), F32),
            pltpu.VMEM((16, rows), F32),
        ],
        4 * 10**9,
    )(seen, weight, cell, slot, inner, outer, factors, loc, low, pert, direction, residual)


def update_kernel(
    sums_ref, control_ref, res_ref, dir_ref, img_ref, control_out, res_out, dir_out, new_ref, sems
):
    members, cols, rows = dir_ref.shape
    total = jnp.sum(sums_ref[...], axis=0, keepdims=True)
    lane = lax.broadcasted_iota(jnp.int32, (1, 128), 1)

    def lane_of(i):
        return jnp.sum(jnp.where(lane == i, total, 0.0), axis=1, keepdims=True)

    norm_old, curvature, cross_term, square = (lane_of(i) for i in range(4))
    step_size = norm_old / curvature
    norm_new = norm_old - 2.0 * step_size * cross_term + step_size * step_size * square
    ratio = norm_new / norm_old
    copies = []
    for m in range(members):
        way = dir_ref[m]
        left = res_ref[m] - step_size * img_ref[m]
        new_ref[0, m] = control_ref[m] + step_size * way
        new_ref[1, m] = left
        new_ref[2, m] = left + ratio * way
        for i, out in enumerate((control_out, res_out, dir_out)):
            copy = pltpu.make_async_copy(new_ref.at[i, m], out.at[m], sems.at[3 * m + i])
            copy.start()
            copies.append(copy)
    for copy in copies:
        copy.wait()


def updated(sums, control, residual, direction, image):
    members = control.shape[0]
    return call(
        update_kernel,
        "update",
        [floats(*control.shape)] * 3,
        [pltpu.VMEM((3, *control.shape), F32), pltpu.SemaphoreType.DMA((3 * members,))],
        10**7,
        out_specs=[HBM, HBM, HBM],
    )(sums, control, residual, direction, image)


def swapped(inner, outer):
    count = lax.axis_size(LON)
    inner_pairs = [(i, i ^ 1) for i in range(count)]
    outer_pairs = [(i, ((i + 1) ^ 1) - 1) for i in range(count)]
    outer_pairs = [(source, target % count) for source, target in outer_pairs]
    return lax.ppermute(inner, LON, inner_pairs), lax.ppermute(outer, LON, outer_pairs)


def body(control, residual, direction, ens_perturb, localize, obs_cell, obs_slot, obs_weight):
    cols = control.shape[2]
    factors = jnp.asarray(grid_factors(localize.shape[0]))
    turned = lambda x: jnp.swapaxes(x, 1, 2)
    control_t, residual_t, direction_t = turned(control), turned(residual), turned(direction)
    pert = jnp.swapaxes(ens_perturb, 2, 3)
    cell, slot, weight = obs_cell[None], obs_slot[None], obs_weight[None]
    lists = [x.reshape(-1, 128) for x in (obs_cell, obs_slot, obs_weight)]
    inc, inner, outer, loc, low = partial_increment(localize, direction_t, pert, lists)
    inner, outer = swapped(inner, outer)
    seen = inner_observed(inc, factors, cell, slot)
    seen = observed_parts(seen, inc, inner, outer, factors, cell, slot, lax.axis_size(ENS))
    seen = lax.all_to_all(seen, ENS, 0, 0, tiled=True)
    image, sums = image_and_sums(
        seen, weight, cell, slot, inner, outer, factors, loc, low, pert, direction_t, residual_t,
        lax.axis_size(ENS_LON),
    )
    sums = lax.all_to_all(sums, ENS_LON, 0, 0, tiled=True)
    results = updated(sums, control_t, residual_t, direction_t, image)
    return tuple(turned(x) for x in results)


def solution(mesh):
    split = Mesh(mesh.devices.reshape(2, 4, 8, 2, 2), ("ens_0", "ens_1", "lon_0", "lon_1", "lon_2"))
    placed = (
        P(ENS, None, LON),
        P(ENS, None, LON),
        P(ENS, None, LON),
        P(ENS, None, None, LON),
        P(),
        P(LON),
        P(LON),
        P(LON),
    )
    return jax.shard_map(
        body,
        mesh=split,
        in_specs=placed,
        out_specs=(P(ENS, None, LON), P(ENS, None, LON), P(ENS, None, LON)),
        check_vma=False,
    )
```

```python
import jax
import jax.numpy as jnp
import numpy as np
from jax import lax
from jax.experimental import pallas as pl
from jax.experimental.pallas import tpu as pltpu
from jax.sharding import Mesh
from jax.sharding import PartitionSpec as P

STEPS = 3
HALO = 3
PAD = 8
LON = ("lon_0", "lon_1", "lon_2")
ENS = ("ens_0", "ens_1")
ENS_LON = ("ens_0", "ens_1", "lon_0", "lon_1", "lon_2")

wave_speed = 0.35
rotation = 0.2

F32 = jnp.float32
BF16 = jnp.bfloat16
NT = (((1,), (1,)), ((), ()))
NN = (((1,), (0,)), ((), ()))
HBM = pl.BlockSpec(memory_space=pltpu.HBM)


def split_two(x):
    high = x.astype(BF16)
    low = (x - high.astype(F32)).astype(BF16)
    return high, low


def remainder(x):
    return x - x.astype(BF16).astype(F32)


def dot(a, b, dims):
    return lax.dot_general(a, b, dims, preferred_element_type=F32)


def grid_factors(lat_total):
    row_ids = np.arange(lat_total).astype(np.float32)
    latitude = (-1.0 / 3.0 + 2.0 / 3.0 * (row_ids + 0.5) / lat_total) * np.pi
    return np.stack([1.0 / np.cos(latitude), np.sin(latitude)]).astype(np.float32)


def differences(shape, orient, metric):
    wide, rows = shape
    lane = lax.broadcasted_iota(jnp.int32, (1, rows), 1)
    lon_scale = (orient * wave_speed * 0.5) * metric
    lat_scale = orient * wave_speed * 0.5
    keep_next = jnp.where(lane == rows - 1, 0.0, lat_scale)
    keep_last = jnp.where(lane == 0, 0.0, lat_scale)

    def lon_diff(x):
        return lon_scale * (pltpu.roll(x, wide - 1, 0) - pltpu.roll(x, 1, 0))

    def lat_diff(x):
        return keep_next * pltpu.roll(x, rows - 1, 1) - keep_last * pltpu.roll(x, 1, 1)

    return lon_diff, lat_diff


def model_step(h, u, v, orient, metric, coriolis):
    turn = (orient * rotation) * coriolis
    lon_diff, lat_diff = differences(h.shape, orient, metric)
    return (
        h - (lon_diff(u) + lat_diff(v)),
        u - lon_diff(h) + turn * v,
        v - lat_diff(h) - turn * u,
    )


def first_step(h, orient, metric):
    lon_diff, lat_diff = differences(h.shape, orient, metric)
    return h, -lon_diff(h), -lat_diff(h)


def call(kernel, name, out_shape, scratch, flops, limit_mib=24, **options):
    return pl.pallas_call(
        kernel,
        name=name,
        out_shape=out_shape,
        scratch_shapes=scratch,
        compiler_params=pltpu.CompilerParams(vmem_limit_bytes=limit_mib << 20),
        cost_estimate=pl.CostEstimate(flops=flops, bytes_accessed=1 << 20, transcendentals=0),
        **options,
    )


def floats(*dims):
    return jax.ShapeDtypeStruct(dims, F32)


def rows_and_spots(cell, slot, cols):
    bits = cols.bit_length() - 1
    assert cols == 1 << bits
    return lax.shift_right_logical(cell, bits), slot, cell & (cols - 1)


def one_hot_rows(row, rows):
    ids = lax.broadcasted_iota(jnp.int16, (rows, row.shape[1]), 0)
    return jnp.where(ids == row.astype(jnp.int16), jnp.ones((), BF16), jnp.zeros((), BF16))


def on_odd_tile():
    return lax.axis_index("lon_2") == 1


def put_edge(ref, field, lanes, value):
    for i in range(lanes // 128, lanes // 128 + value.shape[1] // 128):
        line = 3 * HALO * i + HALO * field
        at = i * 128 - lanes
        ref[line : line + HALO] = value[:, at : at + 128]


def get_edge(ref, field):
    tiles = range(ref.shape[0] // (3 * HALO))
    lines = [3 * HALO * i + HALO * field for i in tiles]
    return jnp.concatenate([ref[line : line + HALO] for line in lines], axis=1)


def edge_floats(rows):
    return floats(3 * HALO * rows // 128, 128)


def increment_kernel(
    loc_hbm, dir_hbm, pert_hbm, inc_ref, inner_ref, outer_ref, loc_ref, low_ref,
    dir_ref, pert_ref, parts_ref, sems,
):
    members, cols, rows = dir_ref.shape
    lines = members * cols
    block = 256
    blocks = rows // block
    first = pltpu.make_async_copy(dir_hbm, dir_ref, sems.at[0])
    second = pltpu.make_async_copy(pert_hbm, pert_ref, sems.at[1])
    places = [slice(i * block, (i + 1) * block) for i in range(blocks)]
    copies = [
        pltpu.make_async_copy(loc_hbm.at[here], loc_ref.at[here], sems.at[2 + i])
        for i, here in enumerate(places)
    ]
    odd = on_odd_tile()
    first.start()
    copies[0].start()
    second.start()
    for copy in copies[1:]:
        copy.start()
    first.wait()
    flat = dir_ref[...].reshape(lines, rows)
    parts_ref[0:lines] = flat
    parts_ref[lines : 2 * lines] = remainder(flat)
    for i in range(blocks + 1):
        if i < blocks:
            copies[i].wait()
            low_ref[places[i]] = remainder(loc_ref[places[i]]).astype(BF16)
        if i == 0:
            continue
        if i == 1:
            second.wait()
        here = places[i - 1]
        both = dot(parts_ref[...], loc_ref[here], NT)
        rest = dot(parts_ref[0:lines].astype(BF16), low_ref[here], NT)
        localized = both[0:lines] + both[lines : 2 * lines] + rest
        for field in range(3):
            total = None
            for m in range(members):
                term = pert_ref[m, field, :, here].astype(F32) * localized[m * cols : (m + 1) * cols]
                total = term if total is None else total + term
            inc_ref[field, :, here] = total
            west, east = total[0:HALO], total[cols - HALO : cols]
            put_edge(inner_ref, field, here.start, jnp.where(odd, west, east))
            put_edge(outer_ref, field, here.start, jnp.where(odd, east, west))


def partial_increment(localize, direction, pert):
    members, cols, rows = direction.shape
    low = jax.ShapeDtypeStruct((rows, rows), BF16)
    return call(
        increment_kernel,
        "increment",
        [floats(3, cols, rows), edge_floats(rows), edge_floats(rows), floats(rows, rows), low],
        [
            pltpu.VMEM(direction.shape, F32),
            pltpu.VMEM(pert.shape, BF16),
            pltpu.VMEM((2 * members * cols, rows), F32),
            pltpu.SemaphoreType.DMA((2 + rows // 256,)),
        ],
        10**9,
        in_specs=[HBM, HBM, HBM],
    )(*(pltpu.with_memory_space_constraint(x, pltpu.HBM) for x in (localize, direction, pert)))


def forward_steps(state_ref, factor_ref, parts_ref, places):
    metric = factor_ref[0:1]
    coriolis = factor_ref[1:2]
    count = sum(stop - start for start, stop in places)
    for moment in range(STEPS):
        h, u, v = model_step(state_ref[0], state_ref[1], state_ref[2], 1.0, metric, coriolis)
        if moment + 1 < STEPS:
            state_ref[0] = h
            state_ref[1] = u
            state_ref[2] = v
        line = moment * count
        for start, stop in places:
            high, low = split_two(h[start:stop])
            parts_ref[line : line + stop - start] = high
            parts_ref[STEPS * count + line : STEPS * count + line + stop - start] = low
            line += stop - start


def sampled(parts_ref, row, spot, rows):
    spots = parts_ref.shape[0] // 2
    picked = dot(parts_ref[...], one_hot_rows(row, rows), NN)
    picked = picked[0:spots] + picked[spots : 2 * spots]
    spot_hot = lax.broadcasted_iota(jnp.int32, picked.shape, 0) == spot
    return jnp.sum(jnp.where(spot_hot, picked, 0.0), axis=0, keepdims=True)


def forward_kernel(inc_ref, factor_ref, cell_ref, slot_ref, out_ref, state_ref, parts_ref):
    _, cols, rows = inc_ref.shape
    nobs = cell_ref.shape[1]
    state_ref[...] = inc_ref[...]
    forward_steps(state_ref, factor_ref, parts_ref, ((PAD, cols - PAD),))
    chunk = 512
    for start in range(0, nobs, chunk):
        here = slice(start, start + chunk)
        row, slot, col = rows_and_spots(cell_ref[:, here], slot_ref[:, here], cols)
        within = (col >= PAD) & (col < cols - PAD)
        spot = jnp.where(within, slot * (cols - 2 * PAD) + (col - PAD), -1)
        out_ref[:, here] = sampled(parts_ref, row, spot, rows)


def inner_observed(inc, factors, cell, slot):
    _, cols, rows = inc.shape
    return call(
        forward_kernel,
        "forward",
        floats(1, cell.shape[1]),
        [
            pltpu.VMEM((3, cols, rows), F32),
            pltpu.VMEM((2 * STEPS * (cols - 2 * PAD), rows), BF16),
        ],
        4 * 10**9,
    )(inc, factors, cell, slot)


def border_kernel(
    seen_ref, inc_ref, inner_ref, outer_ref, factor_ref, cell_ref, slot_ref, out_ref,
    state_ref, parts_ref,
):
    _, cols, rows = inc_ref.shape
    nobs = cell_ref.shape[1]
    odd = on_odd_tile()
    state_ref[...] = jnp.zeros(state_ref.shape, F32)
    for field in range(3):
        inner, outer = get_edge(inner_ref, field), get_edge(outer_ref, field)
        state_ref[field, PAD - HALO : PAD] = jnp.where(odd, inner, outer)
        state_ref[field, PAD : 3 * PAD] = inc_ref[field, 0 : 2 * PAD]
        state_ref[field, 3 * PAD : 5 * PAD] = inc_ref[field, cols - 2 * PAD : cols]
        state_ref[field, 5 * PAD : 5 * PAD + HALO] = jnp.where(odd, outer, inner)
    forward_steps(state_ref, factor_ref, parts_ref, ((PAD, 2 * PAD), (4 * PAD, 5 * PAD)))
    near = 2 * PAD
    chunk = 512
    for start in range(0, nobs, chunk):
        here = slice(start, start + chunk)
        row, slot, col = rows_and_spots(cell_ref[:, here], slot_ref[:, here], cols)
        east_spot = jnp.where(col >= cols - PAD, slot * near + (col - cols + near), -1)
        spot = jnp.where(col < PAD, slot * near + col, east_spot)
        value = sampled(parts_ref, row, spot, rows) + seen_ref[:, here]
        for i in range(0, chunk, 128):
            line = (start + i) // 128
            out_ref[:, line, :] = jnp.broadcast_to(value[:, i : i + 128], (out_ref.shape[0], 128))


def observed_parts(seen, inc, inner, outer, factors, cell, slot, copies):
    rows = inc.shape[2]
    return call(
        border_kernel,
        "border",
        floats(copies, cell.shape[1] // 128, 128),
        [
            pltpu.VMEM((3, 6 * PAD, rows), F32),
            pltpu.VMEM((4 * STEPS * PAD, rows), BF16),
        ],
        10**9,
    )(seen, inc, inner, outer, factors, cell, slot)


def backward_steps(state_ref, factor_ref, add_force):
    metric = factor_ref[0:1]
    coriolis = factor_ref[1:2]
    state_ref[0] = jnp.zeros(state_ref.shape[1:], F32)
    for moment in reversed(range(STEPS)):
        add_force(moment)
        if moment == STEPS - 1:
            h, u, v = first_step(state_ref[0], -1.0, metric)
        else:
            h, u, v = model_step(state_ref[0], state_ref[1], state_ref[2], -1.0, metric, coriolis)
        state_ref[0] = h
        state_ref[1] = u
        state_ref[2] = v


def placed(spots, spot, weighted):
    spot_hot = lax.broadcasted_iota(jnp.int32, (spots, spot.shape[1]), 0) == spot
    return jnp.concatenate(split_two(jnp.where(spot_hot, weighted, 0.0)), axis=0)


def gather_force(force_ref, part, start):
    spots = force_ref.shape[0]
    part = part[0:spots] + part[spots : 2 * spots]
    if start == 0:
        force_ref[...] = part
    else:
        force_ref[...] += part


def edge_adjoint_kernel(
    seen_ref, weight_ref, cell_ref, slot_ref, lines_ref, factor_ref,
    weighted_ref, force_ref, inner_ref, outer_ref, state_ref, *, cols,
):
    rows = factor_ref.shape[1]
    nobs = cell_ref.shape[1]
    near = 2 * PAD
    chunk = 512
    seen = jnp.sum(seen_ref[...], axis=0)
    upright = jnp.transpose(lax.shift_right_logical(lines_ref[...], cols.bit_length() - 1))
    ids = lax.broadcasted_iota(jnp.int16, (128, rows), 1)
    for start in range(0, nobs, chunk):
        here = slice(start, start + chunk)
        _, slot, col = rows_and_spots(cell_ref[:, here], slot_ref[:, here], cols)
        lines = range(start // 128, (start + chunk) // 128)
        weighted = weight_ref[:, here] * jnp.concatenate([seen[i : i + 1] for i in lines], axis=1)
        weighted_ref[:, here] = weighted
        east_spot = jnp.where(col >= cols - PAD, slot * near + (col - cols + near), -1)
        spot = jnp.where(col < PAD, slot * near + col, east_spot)
        hots = []
        for i in lines:
            row = jnp.broadcast_to(upright[:, i : i + 1], (128, 128)).astype(jnp.int16)
            row = jnp.concatenate([row] * (rows // 128), axis=1)
            hots.append(jnp.where(ids == row, jnp.ones((), BF16), jnp.zeros((), BF16)))
        part = dot(placed(STEPS * near, spot, weighted), jnp.concatenate(hots, axis=0), NN)
        gather_force(force_ref, part, start)

    def add_force(moment):
        state_ref[0, PAD : 3 * PAD] += force_ref[moment * near : (moment + 1) * near]

    backward_steps(state_ref, factor_ref, add_force)
    odd = on_odd_tile()
    for field in range(3):
        west = state_ref[field, PAD - HALO : PAD]
        east = state_ref[field, 3 * PAD : 3 * PAD + HALO]
        put_edge(inner_ref, field, 0, jnp.where(odd, west, east))
        put_edge(outer_ref, field, 0, jnp.where(odd, east, west))


def edge_adjoint(seen, weight, cell, slot, factors, cols):
    rows = factors.shape[1]
    nobs = cell.shape[1]
    return call(
        lambda *refs: edge_adjoint_kernel(*refs, cols=cols),
        "edge_adjoint",
        [floats(1, nobs), floats(2 * STEPS * PAD, rows), edge_floats(rows), edge_floats(rows)],
        [pltpu.VMEM((3, 4 * PAD, rows), F32)],
        10**9,
    )(seen, weight, cell, slot, cell.reshape(nobs // 128, 128), factors)


def three_products(parts_ref, loc_ref, low_ref, lines):
    both = dot(parts_ref[...], loc_ref[...], NN)
    rest = dot(parts_ref[0:lines].astype(BF16), low_ref[...], NN)
    return both[0:lines] + both[lines : 2 * lines] + rest


def adjoint_kernel(
    weighted_ref, edge_ref, cell_ref, slot_ref, factor_ref, adj_ref, state_ref, force_ref
):
    _, cols, rows = adj_ref.shape
    nobs = cell_ref.shape[1]
    count = cols - 2 * PAD
    chunk = 512
    for start in range(0, nobs, chunk):
        here = slice(start, start + chunk)
        row, slot, col = rows_and_spots(cell_ref[:, here], slot_ref[:, here], cols)
        within = (col >= PAD) & (col < cols - PAD)
        spot = jnp.where(within, slot * count + (col - PAD), -1)
        hot = placed(STEPS * count, spot, weighted_ref[:, here])
        gather_force(force_ref, dot(hot, one_hot_rows(row, rows), NT), start)

    def add_force(moment):
        near = 2 * PAD * moment
        state_ref[0, PAD : 2 * PAD] += edge_ref[near : near + PAD]
        state_ref[0, 2 * PAD : cols] += force_ref[moment * count : (moment + 1) * count]
        state_ref[0, cols : PAD + cols] += edge_ref[near + PAD : near + 2 * PAD]

    backward_steps(state_ref, factor_ref, add_force)
    for field in range(3):
        adj_ref[field] = state_ref[field, PAD : PAD + cols]


def tile_adjoint(weighted, edge, cell, slot, factors, cols):
    rows = factors.shape[1]
    return call(
        adjoint_kernel,
        "adjoint",
        floats(3, cols, rows),
        [
            pltpu.VMEM((3, cols + 2 * PAD, rows), F32),
            pltpu.VMEM((STEPS * (cols - 2 * PAD), rows), F32),
        ],
        4 * 10**9,
    )(weighted, edge, cell, slot, factors)


def image_kernel(
    loc_ref, low_ref, adj_ref, inner_ref, outer_ref, pert_ref, dir_ref, res_ref,
    img_ref, sums_ref, full_ref, parts_ref,
):
    members, cols, rows = dir_ref.shape
    lines = members * cols
    odd = on_odd_tile()
    full_ref[...] = adj_ref[...]
    for field in range(3):
        inner, outer = get_edge(inner_ref, field), get_edge(outer_ref, field)
        full_ref[field, 0:HALO] += jnp.where(odd, inner, outer)
        full_ref[field, cols - HALO : cols] += jnp.where(odd, outer, inner)
    for m in range(members):
        projected = pert_ref[m, 0].astype(F32) * full_ref[0]
        projected += pert_ref[m, 1].astype(F32) * full_ref[1]
        projected += pert_ref[m, 2].astype(F32) * full_ref[2]
        parts_ref[m * cols : (m + 1) * cols] = projected
        parts_ref[lines + m * cols : lines + (m + 1) * cols] = remainder(projected)
    pulled = three_products(parts_ref, loc_ref, low_ref, lines)
    img_ref[...] = dir_ref[...] + pulled.reshape(members, cols, rows)
    totals = [jnp.zeros((8, rows), F32) for _ in range(4)]
    for m in range(members):
        for start in range(0, cols, 8):
            here = slice(start, start + 8)
            image, way, left = img_ref[m, here], dir_ref[m, here], res_ref[m, here]
            totals[0] += left * left
            totals[1] += way * image
            totals[2] += left * image
            totals[3] += image * image
    lane = lax.broadcasted_iota(jnp.int32, (1, 128), 1)
    packed = jnp.zeros((1, 128), F32)
    for i in range(4):
        total = jnp.sum(jnp.sum(totals[i], axis=0, keepdims=True), axis=1, keepdims=True)
        packed = jnp.where(lane == i, total, packed)
    sums_ref[...] = jnp.broadcast_to(packed, sums_ref.shape)


def image_and_sums(loc, low, adj, inner, outer, pert, direction, residual, copies):
    members, cols, rows = direction.shape
    return call(
        image_kernel,
        "image",
        [floats(members, cols, rows), floats(copies, 128)],
        [
            pltpu.VMEM((3, cols, rows), F32),
            pltpu.VMEM((2 * members * cols, rows), F32),
        ],
        10**9,
    )(loc, low, adj, inner, outer, pert, direction, residual)


def update_kernel(
    sums_ref, control_ref, res_ref, dir_ref, img_ref, control_out, res_out, dir_out, new_ref, sems
):
    members, cols, rows = dir_ref.shape
    total = jnp.sum(sums_ref[...], axis=0, keepdims=True)
    lane = lax.broadcasted_iota(jnp.int32, (1, 128), 1)

    def lane_of(i):
        return jnp.sum(jnp.where(lane == i, total, 0.0), axis=1, keepdims=True)

    norm_old, curvature, cross_term, square = (lane_of(i) for i in range(4))
    step_size = norm_old / curvature
    norm_new = norm_old - 2.0 * step_size * cross_term + step_size * step_size * square
    ratio = norm_new / norm_old
    copies = []
    for m in range(members):
        way = dir_ref[m]
        left = res_ref[m] - step_size * img_ref[m]
        new_ref[0, m] = control_ref[m] + step_size * way
        new_ref[1, m] = left
        new_ref[2, m] = left + ratio * way
        for i, out in enumerate((control_out, res_out, dir_out)):
            copy = pltpu.make_async_copy(new_ref.at[i, m], out.at[m], sems.at[3 * m + i])
            copy.start()
            copies.append(copy)
    for copy in copies:
        copy.wait()


def updated(sums, control, residual, direction, image):
    members = control.shape[0]
    return call(
        update_kernel,
        "update",
        [floats(*control.shape)] * 3,
        [pltpu.VMEM((3, *control.shape), F32), pltpu.SemaphoreType.DMA((3 * members,))],
        10**7,
        out_specs=[HBM, HBM, HBM],
    )(sums, control, residual, direction, image)


def swapped(inner, outer):
    count = lax.axis_size(LON)
    inner_pairs = [(i, i ^ 1) for i in range(count)]
    outer_pairs = [(i, ((i + 1) ^ 1) - 1) for i in range(count)]
    outer_pairs = [(source, target % count) for source, target in outer_pairs]
    return lax.ppermute(inner, LON, inner_pairs), lax.ppermute(outer, LON, outer_pairs)


def body(control, residual, direction, ens_perturb, localize, obs_cell, obs_slot, obs_weight):
    cols = control.shape[2]
    factors = jnp.asarray(grid_factors(localize.shape[0]))
    turned = lambda x: jnp.swapaxes(x, 1, 2)
    control_t, residual_t, direction_t = turned(control), turned(residual), turned(direction)
    pert = jnp.swapaxes(ens_perturb, 2, 3)
    cell, slot, weight = obs_cell[None], obs_slot[None], obs_weight[None]
    inc, inner, outer, loc, low = partial_increment(localize, direction_t, pert)
    inner, outer = swapped(inner, outer)
    seen = inner_observed(inc, factors, cell, slot)
    seen = observed_parts(seen, inc, inner, outer, factors, cell, slot, lax.axis_size(ENS))
    seen = lax.all_to_all(seen, ENS, 0, 0, tiled=True)
    weighted, edge, inner, outer = edge_adjoint(seen, weight, cell, slot, factors, cols)
    inner, outer = swapped(inner, outer)
    adj = tile_adjoint(weighted, edge, cell, slot, factors, cols)
    image, sums = image_and_sums(
        loc, low, adj, inner, outer, pert, direction_t, residual_t, lax.axis_size(ENS_LON)
    )
    sums = lax.all_to_all(sums, ENS_LON, 0, 0, tiled=True)
    results = updated(sums, control_t, residual_t, direction_t, image)
    return tuple(turned(x) for x in results)


def solution(mesh):
    split = Mesh(mesh.devices.reshape(2, 4, 8, 2, 2), ("ens_0", "ens_1", "lon_0", "lon_1", "lon_2"))
    placed = (
        P(ENS, None, LON),
        P(ENS, None, LON),
        P(ENS, None, LON),
        P(ENS, None, None, LON),
        P(),
        P(LON),
        P(LON),
        P(LON),
    )
    return jax.shard_map(
        body,
        mesh=split,
        in_specs=placed,
        out_specs=(P(ENS, None, LON), P(ENS, None, LON), P(ENS, None, LON)),
        check_vma=False,
    )
```

```python
import jax
import jax.numpy as jnp
import numpy as np
from jax import lax
from jax.experimental import pallas as pl
from jax.experimental.pallas import tpu as pltpu
from jax.sharding import Mesh
from jax.sharding import PartitionSpec as P

STEPS = 3
HALO = 3
PAD = 8
LON = ("lon_0", "lon_1", "lon_2")
ENS = ("ens_0", "ens_1")
ENS_LON = ("ens_0", "ens_1", "lon_0", "lon_1", "lon_2")

wave_speed = 0.35
rotation = 0.2

F32 = jnp.float32
BF16 = jnp.bfloat16
NT = (((1,), (1,)), ((), ()))
NN = (((1,), (0,)), ((), ()))
HBM = pl.BlockSpec(memory_space=pltpu.HBM)


def split_two(x):
    high = x.astype(BF16)
    low = (x - high.astype(F32)).astype(BF16)
    return high, low


def remainder(x):
    return x - x.astype(BF16).astype(F32)


def dot(a, b, dims):
    return lax.dot_general(a, b, dims, preferred_element_type=F32)


def grid_factors(lat_total):
    row_ids = np.arange(lat_total).astype(np.float32)
    latitude = (-1.0 / 3.0 + 2.0 / 3.0 * (row_ids + 0.5) / lat_total) * np.pi
    return np.stack([1.0 / np.cos(latitude), np.sin(latitude)]).astype(np.float32)


def differences(shape, orient, metric):
    wide, rows = shape
    lane = lax.broadcasted_iota(jnp.int32, (1, rows), 1)
    lon_scale = (orient * wave_speed * 0.5) * metric
    lat_scale = orient * wave_speed * 0.5
    keep_next = jnp.where(lane == rows - 1, 0.0, lat_scale)
    keep_last = jnp.where(lane == 0, 0.0, lat_scale)

    def lon_diff(x):
        return lon_scale * (pltpu.roll(x, wide - 1, 0) - pltpu.roll(x, 1, 0))

    def lat_diff(x):
        return keep_next * pltpu.roll(x, rows - 1, 1) - keep_last * pltpu.roll(x, 1, 1)

    return lon_diff, lat_diff


def model_step(h, u, v, orient, metric, coriolis):
    turn = (orient * rotation) * coriolis
    lon_diff, lat_diff = differences(h.shape, orient, metric)
    return (
        h - (lon_diff(u) + lat_diff(v)),
        u - lon_diff(h) + turn * v,
        v - lat_diff(h) - turn * u,
    )


def first_step(h, orient, metric):
    lon_diff, lat_diff = differences(h.shape, orient, metric)
    return h, -lon_diff(h), -lat_diff(h)


def call(kernel, out_shape, scratch, flops, limit_mib=24, **options):
    return pl.pallas_call(
        kernel,
        out_shape=out_shape,
        scratch_shapes=scratch,
        compiler_params=pltpu.CompilerParams(vmem_limit_bytes=limit_mib << 20),
        cost_estimate=pl.CostEstimate(flops=flops, bytes_accessed=1 << 20, transcendentals=0),
        **options,
    )


def floats(*dims):
    return jax.ShapeDtypeStruct(dims, F32)


def rows_and_spots(cell, slot, cols):
    bits = cols.bit_length() - 1
    assert cols == 1 << bits
    return lax.shift_right_logical(cell, bits), slot, cell & (cols - 1)


def one_hot_rows(row, rows):
    ids = lax.broadcasted_iota(jnp.int16, (rows, row.shape[1]), 0)
    return jnp.where(ids == row.astype(jnp.int16), jnp.ones((), BF16), jnp.zeros((), BF16))


def on_odd_tile():
    return lax.axis_index("lon_2") == 1


def put_edge(ref, field, lanes, value):
    for i in range(lanes // 128, lanes // 128 + value.shape[1] // 128):
        line = 3 * HALO * i + HALO * field
        at = i * 128 - lanes
        ref[line : line + HALO] = value[:, at : at + 128]


def get_edge(ref, field):
    tiles = range(ref.shape[0] // (3 * HALO))
    lines = [3 * HALO * i + HALO * field for i in tiles]
    return jnp.concatenate([ref[line : line + HALO] for line in lines], axis=1)


def edge_floats(rows):
    return floats(3 * HALO * rows // 128, 128)


def increment_kernel(
    loc_hbm, dir_hbm, pert_hbm, inc_ref, inner_ref, outer_ref, loc_ref, low_ref,
    dir_ref, pert_ref, parts_ref, sems,
):
    members, cols, rows = dir_ref.shape
    lines = members * cols
    block = 256
    blocks = rows // block
    first = pltpu.make_async_copy(dir_hbm, dir_ref, sems.at[0])
    second = pltpu.make_async_copy(pert_hbm, pert_ref, sems.at[1])
    places = [slice(i * block, (i + 1) * block) for i in range(blocks)]
    copies = [
        pltpu.make_async_copy(loc_hbm.at[here], loc_ref.at[here], sems.at[2 + i])
        for i, here in enumerate(places)
    ]
    odd = on_odd_tile()
    first.start()
    copies[0].start()
    second.start()
    for copy in copies[1:]:
        copy.start()
    first.wait()
    flat = dir_ref[...].reshape(lines, rows)
    parts_ref[0:lines] = flat
    parts_ref[lines : 2 * lines] = remainder(flat)
    for i in range(blocks + 1):
        if i < blocks:
            copies[i].wait()
            low_ref[places[i]] = remainder(loc_ref[places[i]]).astype(BF16)
        if i == 0:
            continue
        if i == 1:
            second.wait()
        here = places[i - 1]
        both = dot(parts_ref[...], loc_ref[here], NT)
        rest = dot(parts_ref[0:lines].astype(BF16), low_ref[here], NT)
        localized = both[0:lines] + both[lines : 2 * lines] + rest
        for field in range(3):
            total = None
            for m in range(members):
                term = pert_ref[m, field, :, here].astype(F32) * localized[m * cols : (m + 1) * cols]
                total = term if total is None else total + term
            inc_ref[field, :, here] = total
            west, east = total[0:HALO], total[cols - HALO : cols]
            put_edge(inner_ref, field, here.start, jnp.where(odd, west, east))
            put_edge(outer_ref, field, here.start, jnp.where(odd, east, west))


def partial_increment(localize, direction, pert):
    members, cols, rows = direction.shape
    low = jax.ShapeDtypeStruct((rows, rows), BF16)
    return call(
        increment_kernel,
        [floats(3, cols, rows), edge_floats(rows), edge_floats(rows), floats(rows, rows), low],
        [
            pltpu.VMEM(direction.shape, F32),
            pltpu.VMEM(pert.shape, BF16),
            pltpu.VMEM((2 * members * cols, rows), F32),
            pltpu.SemaphoreType.DMA((2 + rows // 256,)),
        ],
        10**9,
        in_specs=[HBM, HBM, HBM],
    )(*(pltpu.with_memory_space_constraint(x, pltpu.HBM) for x in (localize, direction, pert)))


def forward_steps(state_ref, factor_ref, parts_ref, places):
    metric = factor_ref[0:1]
    coriolis = factor_ref[1:2]
    count = sum(stop - start for start, stop in places)
    for moment in range(STEPS):
        h, u, v = model_step(state_ref[0], state_ref[1], state_ref[2], 1.0, metric, coriolis)
        if moment + 1 < STEPS:
            state_ref[0] = h
            state_ref[1] = u
            state_ref[2] = v
        line = moment * count
        for start, stop in places:
            high, low = split_two(h[start:stop])
            parts_ref[line : line + stop - start] = high
            parts_ref[STEPS * count + line : STEPS * count + line + stop - start] = low
            line += stop - start


def sampled(parts_ref, row, spot, rows):
    spots = parts_ref.shape[0] // 2
    picked = dot(parts_ref[...], one_hot_rows(row, rows), NN)
    picked = picked[0:spots] + picked[spots : 2 * spots]
    spot_hot = lax.broadcasted_iota(jnp.int32, picked.shape, 0) == spot
    return jnp.sum(jnp.where(spot_hot, picked, 0.0), axis=0, keepdims=True)


def forward_kernel(inc_ref, factor_ref, cell_ref, slot_ref, out_ref, state_ref, parts_ref):
    _, cols, rows = inc_ref.shape
    nobs = cell_ref.shape[1]
    state_ref[...] = inc_ref[...]
    forward_steps(state_ref, factor_ref, parts_ref, ((PAD, cols - PAD),))
    chunk = 512
    for start in range(0, nobs, chunk):
        here = slice(start, start + chunk)
        row, slot, col = rows_and_spots(cell_ref[:, here], slot_ref[:, here], cols)
        within = (col >= PAD) & (col < cols - PAD)
        spot = jnp.where(within, slot * (cols - 2 * PAD) + (col - PAD), -1)
        out_ref[:, here] = sampled(parts_ref, row, spot, rows)


def inner_observed(inc, factors, cell, slot):
    _, cols, rows = inc.shape
    return call(
        forward_kernel,
        floats(1, cell.shape[1]),
        [
            pltpu.VMEM((3, cols, rows), F32),
            pltpu.VMEM((2 * STEPS * (cols - 2 * PAD), rows), BF16),
        ],
        4 * 10**9,
    )(inc, factors, cell, slot)


def border_kernel(
    seen_ref, inc_ref, inner_ref, outer_ref, factor_ref, cell_ref, slot_ref, out_ref,
    state_ref, parts_ref,
):
    _, cols, rows = inc_ref.shape
    nobs = cell_ref.shape[1]
    odd = on_odd_tile()
    state_ref[...] = jnp.zeros(state_ref.shape, F32)
    for field in range(3):
        inner, outer = get_edge(inner_ref, field), get_edge(outer_ref, field)
        state_ref[field, PAD - HALO : PAD] = jnp.where(odd, inner, outer)
        state_ref[field, PAD : 3 * PAD] = inc_ref[field, 0 : 2 * PAD]
        state_ref[field, 3 * PAD : 5 * PAD] = inc_ref[field, cols - 2 * PAD : cols]
        state_ref[field, 5 * PAD : 5 * PAD + HALO] = jnp.where(odd, outer, inner)
    forward_steps(state_ref, factor_ref, parts_ref, ((PAD, 2 * PAD), (4 * PAD, 5 * PAD)))
    near = 2 * PAD
    chunk = 512
    for start in range(0, nobs, chunk):
        here = slice(start, start + chunk)
        row, slot, col = rows_and_spots(cell_ref[:, here], slot_ref[:, here], cols)
        east_spot = jnp.where(col >= cols - PAD, slot * near + (col - cols + near), -1)
        spot = jnp.where(col < PAD, slot * near + col, east_spot)
        value = sampled(parts_ref, row, spot, rows) + seen_ref[:, here]
        for i in range(0, chunk, 128):
            line = (start + i) // 128
            out_ref[:, line, :] = jnp.broadcast_to(value[:, i : i + 128], (out_ref.shape[0], 128))


def observed_parts(seen, inc, inner, outer, factors, cell, slot, copies):
    rows = inc.shape[2]
    return call(
        border_kernel,
        floats(copies, cell.shape[1] // 128, 128),
        [
            pltpu.VMEM((3, 6 * PAD, rows), F32),
            pltpu.VMEM((4 * STEPS * PAD, rows), BF16),
        ],
        10**9,
    )(seen, inc, inner, outer, factors, cell, slot)


def backward_steps(state_ref, factor_ref, add_force):
    metric = factor_ref[0:1]
    coriolis = factor_ref[1:2]
    state_ref[0] = jnp.zeros(state_ref.shape[1:], F32)
    for moment in reversed(range(STEPS)):
        add_force(moment)
        if moment == STEPS - 1:
            h, u, v = first_step(state_ref[0], -1.0, metric)
        else:
            h, u, v = model_step(state_ref[0], state_ref[1], state_ref[2], -1.0, metric, coriolis)
        state_ref[0] = h
        state_ref[1] = u
        state_ref[2] = v


def placed(spots, spot, weighted):
    spot_hot = lax.broadcasted_iota(jnp.int32, (spots, spot.shape[1]), 0) == spot
    return jnp.concatenate(split_two(jnp.where(spot_hot, weighted, 0.0)), axis=0)


def gather_force(force_ref, part, start):
    spots = force_ref.shape[0]
    part = part[0:spots] + part[spots : 2 * spots]
    if start == 0:
        force_ref[...] = part
    else:
        force_ref[...] += part


def edge_adjoint_kernel(
    seen_ref, weight_ref, cell_ref, slot_ref, lines_ref, factor_ref,
    weighted_ref, force_ref, inner_ref, outer_ref, state_ref, *, cols,
):
    rows = factor_ref.shape[1]
    nobs = cell_ref.shape[1]
    near = 2 * PAD
    chunk = 512
    seen = jnp.sum(seen_ref[...], axis=0)
    upright = jnp.transpose(lax.shift_right_logical(lines_ref[...], cols.bit_length() - 1))
    ids = lax.broadcasted_iota(jnp.int16, (128, rows), 1)
    for start in range(0, nobs, chunk):
        here = slice(start, start + chunk)
        _, slot, col = rows_and_spots(cell_ref[:, here], slot_ref[:, here], cols)
        lines = range(start // 128, (start + chunk) // 128)
        weighted = weight_ref[:, here] * jnp.concatenate([seen[i : i + 1] for i in lines], axis=1)
        weighted_ref[:, here] = weighted
        east_spot = jnp.where(col >= cols - PAD, slot * near + (col - cols + near), -1)
        spot = jnp.where(col < PAD, slot * near + col, east_spot)
        hots = []
        for i in lines:
            row = jnp.broadcast_to(upright[:, i : i + 1], (128, 128)).astype(jnp.int16)
            row = jnp.concatenate([row] * (rows // 128), axis=1)
            hots.append(jnp.where(ids == row, jnp.ones((), BF16), jnp.zeros((), BF16)))
        part = dot(placed(STEPS * near, spot, weighted), jnp.concatenate(hots, axis=0), NN)
        gather_force(force_ref, part, start)

    def add_force(moment):
        state_ref[0, PAD : 3 * PAD] += force_ref[moment * near : (moment + 1) * near]

    backward_steps(state_ref, factor_ref, add_force)
    odd = on_odd_tile()
    for field in range(3):
        west = state_ref[field, PAD - HALO : PAD]
        east = state_ref[field, 3 * PAD : 3 * PAD + HALO]
        put_edge(inner_ref, field, 0, jnp.where(odd, west, east))
        put_edge(outer_ref, field, 0, jnp.where(odd, east, west))


def edge_adjoint(seen, weight, cell, slot, factors, cols):
    rows = factors.shape[1]
    nobs = cell.shape[1]
    return call(
        lambda *refs: edge_adjoint_kernel(*refs, cols=cols),
        [floats(1, nobs), floats(2 * STEPS * PAD, rows), edge_floats(rows), edge_floats(rows)],
        [pltpu.VMEM((3, 4 * PAD, rows), F32)],
        10**9,
    )(seen, weight, cell, slot, cell.reshape(nobs // 128, 128), factors)


def three_products(parts_ref, loc_ref, low_ref, lines):
    both = dot(parts_ref[...], loc_ref[...], NN)
    rest = dot(parts_ref[0:lines].astype(BF16), low_ref[...], NN)
    return both[0:lines] + both[lines : 2 * lines] + rest


def adjoint_kernel(
    weighted_ref, edge_ref, cell_ref, slot_ref, factor_ref, loc_ref, low_ref, pert_ref, dir_ref,
    img_ref, state_ref, force_ref, parts_ref,
):
    members, cols, rows = dir_ref.shape
    nobs = cell_ref.shape[1]
    count = cols - 2 * PAD
    chunk = 512
    for start in range(0, nobs, chunk):
        here = slice(start, start + chunk)
        row, slot, col = rows_and_spots(cell_ref[:, here], slot_ref[:, here], cols)
        within = (col >= PAD) & (col < cols - PAD)
        spot = jnp.where(within, slot * count + (col - PAD), -1)
        hot = placed(STEPS * count, spot, weighted_ref[:, here])
        gather_force(force_ref, dot(hot, one_hot_rows(row, rows), NT), start)

    def add_force(moment):
        near = 2 * PAD * moment
        state_ref[0, PAD : 2 * PAD] += edge_ref[near : near + PAD]
        state_ref[0, 2 * PAD : cols] += force_ref[moment * count : (moment + 1) * count]
        state_ref[0, cols : PAD + cols] += edge_ref[near + PAD : near + 2 * PAD]

    backward_steps(state_ref, factor_ref, add_force)
    lines = members * cols
    for m in range(members):
        projected = pert_ref[m, 0].astype(F32) * state_ref[0, PAD : PAD + cols]
        projected += pert_ref[m, 1].astype(F32) * state_ref[1, PAD : PAD + cols]
        projected += pert_ref[m, 2].astype(F32) * state_ref[2, PAD : PAD + cols]
        parts_ref[m * cols : (m + 1) * cols] = projected
        parts_ref[lines + m * cols : lines + (m + 1) * cols] = remainder(projected)
    pulled = three_products(parts_ref, loc_ref, low_ref, lines)
    img_ref[...] = dir_ref[...] + pulled.reshape(members, cols, rows)


def own_image(weighted, edge, cell, slot, factors, loc, low, pert, direction):
    members, cols, rows = direction.shape
    return call(
        adjoint_kernel,
        floats(members, cols, rows),
        [
            pltpu.VMEM((3, cols + 2 * PAD, rows), F32),
            pltpu.VMEM((STEPS * (cols - 2 * PAD), rows), F32),
            pltpu.VMEM((2 * members * cols, rows), F32),
        ],
        4 * 10**9,
    )(weighted, edge, cell, slot, factors, loc, low, pert, direction)


def closing_kernel(
    loc_ref, low_ref, own_ref, inner_ref, outer_ref, pert_ref, dir_ref, res_ref, img_ref, sums_ref,
    edge_ref, parts_ref,
):
    members, cols, rows = dir_ref.shape
    near = 2 * PAD
    lines = members * near
    odd = on_odd_tile()
    edge_ref[...] = jnp.zeros(edge_ref.shape, F32)
    for field in range(3):
        inner, outer = get_edge(inner_ref, field), get_edge(outer_ref, field)
        edge_ref[field, 0:HALO] = jnp.where(odd, inner, outer)
        edge_ref[field, near - HALO : near] = jnp.where(odd, outer, inner)
    for m in range(members):
        west = jnp.zeros((PAD, rows), F32)
        east = jnp.zeros((PAD, rows), F32)
        for field in range(3):
            west += pert_ref[m, field, 0:PAD].astype(F32) * edge_ref[field, 0:PAD]
            east += pert_ref[m, field, cols - PAD : cols].astype(F32) * edge_ref[field, PAD:near]
        projected = jnp.concatenate([west, east], axis=0)
        parts_ref[m * near : (m + 1) * near] = projected
        parts_ref[lines + m * near : lines + (m + 1) * near] = remainder(projected)
    pulled = three_products(parts_ref, loc_ref, low_ref, lines)
    totals = [jnp.zeros((8, rows), F32) for _ in range(4)]
    for m in range(members):
        for start in range(0, cols, PAD):
            here = slice(start, start + PAD)
            image = own_ref[m, here]
            if start == 0:
                image = image + pulled[m * near : m * near + PAD]
            if start == cols - PAD:
                image = image + pulled[m * near + PAD : (m + 1) * near]
            img_ref[m, here] = image
            way = dir_ref[m, here]
            left = res_ref[m, here]
            totals[0] += left * left
            totals[1] += way * image
            totals[2] += left * image
            totals[3] += image * image
    lane = lax.broadcasted_iota(jnp.int32, (1, 128), 1)
    packed = jnp.zeros((1, 128), F32)
    for i in range(4):
        total = jnp.sum(jnp.sum(totals[i], axis=0, keepdims=True), axis=1, keepdims=True)
        packed = jnp.where(lane == i, total, packed)
    sums_ref[...] = jnp.broadcast_to(packed, sums_ref.shape)


def image_and_sums(loc, low, own, inner, outer, pert, direction, residual, copies):
    members, cols, rows = direction.shape
    return call(
        closing_kernel,
        [floats(members, cols, rows), floats(copies, 128)],
        [
            pltpu.VMEM((3, 2 * PAD, rows), F32),
            pltpu.VMEM((4 * members * PAD, rows), F32),
        ],
        5 * 10**8,
    )(loc, low, own, inner, outer, pert, direction, residual)


def update_kernel(
    sums_ref, control_ref, res_ref, dir_ref, img_ref, control_out, res_out, dir_out, new_ref, sems
):
    members, _, _ = dir_ref.shape
    total = jnp.sum(sums_ref[...], axis=0, keepdims=True)
    lane = lax.broadcasted_iota(jnp.int32, (1, 128), 1)

    def lane_of(i):
        return jnp.sum(jnp.where(lane == i, total, 0.0), axis=1, keepdims=True)

    norm_old, curvature, cross_term, square = (lane_of(i) for i in range(4))
    step_size = norm_old / curvature
    norm_new = norm_old - 2.0 * step_size * cross_term + step_size * step_size * square
    ratio = norm_new / norm_old
    copies = []
    for m in range(members):
        way = dir_ref[m]
        left = res_ref[m] - step_size * img_ref[m]
        new_ref[0, m] = control_ref[m] + step_size * way
        new_ref[1, m] = left
        new_ref[2, m] = left + ratio * way
        for i, out in enumerate((control_out, res_out, dir_out)):
            copy = pltpu.make_async_copy(new_ref.at[i, m], out.at[m], sems.at[3 * m + i])
            copy.start()
            copies.append(copy)
    for copy in copies:
        copy.wait()


def updated(sums, control, residual, direction, image):
    members = control.shape[0]
    return call(
        update_kernel,
        [floats(*control.shape)] * 3,
        [pltpu.VMEM((3, *control.shape), F32), pltpu.SemaphoreType.DMA((3 * members,))],
        10**7,
        out_specs=[HBM, HBM, HBM],
    )(sums, control, residual, direction, image)


def swapped(inner, outer):
    count = lax.axis_size(LON)
    inner_pairs = [(i, i ^ 1) for i in range(count)]
    outer_pairs = [(i, ((i + 1) ^ 1) - 1) for i in range(count)]
    outer_pairs = [(source, target % count) for source, target in outer_pairs]
    outer = lax.ppermute(outer, LON, outer_pairs)
    inner = lax.ppermute(inner, LON, inner_pairs)
    return inner, outer


def body(control, residual, direction, ens_perturb, localize, obs_cell, obs_slot, obs_weight):
    cols = control.shape[2]
    factors = jnp.asarray(grid_factors(localize.shape[0]))
    turned = lambda x: jnp.swapaxes(x, 1, 2)
    control_t, residual_t, direction_t = turned(control), turned(residual), turned(direction)
    pert = jnp.swapaxes(ens_perturb, 2, 3)
    cell, slot, weight = obs_cell[None], obs_slot[None], obs_weight[None]
    inc, inner, outer, loc, low = partial_increment(localize, direction_t, pert)
    inner, outer = swapped(inner, outer)
    seen = inner_observed(inc, factors, cell, slot)
    seen = observed_parts(seen, inc, inner, outer, factors, cell, slot, lax.axis_size(ENS))
    seen = lax.all_to_all(seen, ENS, 0, 0, tiled=True)
    weighted, edge, inner, outer = edge_adjoint(seen, weight, cell, slot, factors, cols)
    inner, outer = swapped(inner, outer)
    image = own_image(
        weighted, edge, cell, slot, factors, loc, low, pert, direction_t
    )
    image, sums = image_and_sums(
        loc, low, image, inner, outer, pert, direction_t, residual_t, lax.axis_size(ENS_LON)
    )
    sums = lax.all_to_all(sums, ENS_LON, 0, 0, tiled=True)
    results = updated(sums, control_t, residual_t, direction_t, image)
    return tuple(turned(x) for x in results)


def solution(mesh):
    split = Mesh(mesh.devices.reshape(2, 4, 8, 2, 2), ("ens_0", "ens_1", "lon_0", "lon_1", "lon_2"))
    placed = (
        P(ENS, None, LON),
        P(ENS, None, LON),
        P(ENS, None, LON),
        P(ENS, None, None, LON),
        P(),
        P(LON),
        P(LON),
        P(LON),
    )
    return jax.shard_map(
        body,
        mesh=split,
        in_specs=placed,
        out_specs=(P(ENS, None, LON), P(ENS, None, LON), P(ENS, None, LON)),
        check_vma=False,
    )
```
